32 devices in a mesh: dp: 8 (over z, core), feat: 4 (over y, x).
Axes of the slice: x: 2, y: 2, z: 4, core: 2. Of those that a mesh axis runs over, the one named last changes fastest.
Arguments:
- points: bfloat16 [2048, 256], P('dp'), may hold values from -6 to 6
- freqs: bfloat16 [256, 8192], P(None, 'feat'), may hold values from -0.375 to 0.375
- phase: float32 [8192], P('feat'), may hold values from -3.140625 to 3.140625
- ridge: float32 [8192], P('feat'), may hold values from 0.05 to 0.5
- targets: bfloat16 [8, 2048], P(None, 'dp'), may hold values from -6 to 6
Outputs:
- gram: float32 [8192, 8192], P('feat', 'dp')
- projected: float32 [8, 8192], P(None, 'feat')
- factors: float32 [8192, 1024], P('feat')
The draws below stay inside these ranges and needn't reach their ends.
All inputs are finite; a program needn't handle non-finite values.
Results may differ from the reference program's by a relative error of at most 0.003.
Values may be sent and summed in bfloat16 or wider, within the bound.
A program may use at most 128 MiB of HBM per device.

```python
import math
import jax
import jax.numpy as jnp
from jax import lax

DIN = 256
OUTS = 8
FB = 1024
F = 8192
ROWS = 2048


def steps_of(rng, shape, pieces, smallest, top_value):
    def one(position, blocks):
        steps = jax.random.uniform(jax.random.fold_in(jax.random.fold_in(rng, 6), position), (blocks,), jnp.float32, smallest / len(pieces), top_value / len(pieces))
        return jnp.repeat(jnp.exp(steps), shape[position] // blocks).reshape((-1,) + (1,) * (len(shape) - position - 1))

    gain = one(*pieces[0])
    for cut in pieces[1:]:
        gain = gain * one(*cut)
    return gain


def gaussian(own_key, extent, spread, limit, cuts=(), held_as=jnp.bfloat16):
    array = jax.random.normal(own_key, extent, jnp.float32) * spread
    if len(cuts) > 0:
        array = steps_of(own_key, extent, cuts, -0.22, 0.18) * array
    return jnp.clip(array, min=-limit, max=limit).astype(held_as)


def setup_inputs(seed: int = 0) -> dict:
    keys = jax.random.split(jax.random.key(seed), 6)
    points = gaussian(keys[0], (ROWS, DIN), 1.0, 6.0, ((0, 8),))
    freqs = gaussian(keys[1], (DIN, F), DIN ** -0.5, 0.375, ((1, 4),))
    phase = jnp.clip(jax.random.uniform(keys[2], (F,), jnp.float32, -3.140625, 3.140625), -3.140625, 3.140625)
    ridge = jnp.clip(jnp.exp(math.log(0.5) - 2.3025851 * jax.random.uniform(keys[3], (F,), jnp.float32) ** steps_of(keys[3], (F,), ((0, 4),), -0.2, 0.2)), 0.05, 0.5)
    targets = gaussian(keys[4], (OUTS, ROWS), 1.0, 6.0, ((1, 8),))
    return {"points": points, "freqs": freqs, "phase": phase, "ridge": ridge, "targets": targets}


def reference(points, freqs, phase, ridge, targets):
    scale = math.sqrt(2.0 / ROWS)
    angle = jnp.dot(points.astype(jnp.float32), freqs.astype(jnp.float32), preferred_element_type=jnp.float32) + phase
    phi = (scale * jnp.cos(angle)).astype(jnp.bfloat16)
    phi_wide = phi.astype(jnp.float32)
    gram = jnp.dot(phi_wide.T, phi_wide, precision=lax.Precision.HIGHEST) + jnp.diag(ridge)
    projected = jnp.dot(targets.astype(jnp.float32), phi_wide, precision=lax.Precision.HIGHEST)
    blocks = jnp.stack([gram[block_number * FB:(block_number + 1) * FB, block_number * FB:(block_number + 1) * FB] for block_number in range(OUTS)])
    factors = jnp.linalg.cholesky(blocks).reshape(F, FB)
    return (gram, projected, factors)
```

```python
import functools
import math

import jax
import jax.numpy as jnp
from jax import lax
from jax.experimental import pallas as pl
from jax.experimental.pallas import tpu as pltpu
from jax.sharding import PartitionSpec as P

FB = 1024
TILE = 128
MICRO = 16
WIDE = 256
MIB = 1024 * 1024
COS_TURNS = (
    0.9999991998413438,
    -19.738978175861334,
    64.92858783993428,
    -85.27084362691367,
    58.786940763031694,
    -21.065429407523915,
)


def features(rows, freq_cols, phase_turns, scale):
    angle = jnp.dot(rows, freq_cols, preferred_element_type=jnp.float32)
    return wave(angle * (0.5 / math.pi) + phase_turns, scale)


def wave(turns, scale):
    part = turns - jnp.round(turns)
    square = part * part
    poly = square * (scale * COS_TURNS[-1]) + scale * COS_TURNS[-2]
    for coeff in COS_TURNS[-3::-1]:
        poly = poly * square + scale * coeff
    return poly.astype(jnp.bfloat16)


def cross(left, right):
    return lax.dot_general(
        left, right, (((0,), (0,)), ((), ())), preferred_element_type=jnp.float32
    )


def with_ridge(tile, ridge, row_start, col_start):
    rows_here = row_start + lax.broadcasted_iota(jnp.int32, tile.shape, 0)
    cols_here = col_start + lax.broadcasted_iota(jnp.int32, tile.shape, 1)
    return tile + jnp.where(rows_here == cols_here, ridge, 0.0)


def halves(value):
    high = value.astype(jnp.bfloat16)
    return high, (value - high.astype(jnp.float32)).astype(jnp.bfloat16)


def left_parts(value, axis):
    high, low = halves(value)
    return jnp.concatenate([high, high, low], axis=axis)


def right_parts(value):
    high, low = halves(value)
    return jnp.concatenate([high, low, high], axis=0)


def panel_rows(rows_lead, rows_tail, start):
    shape = rows_lead.shape
    row_ids = lax.broadcasted_iota(jnp.int32, shape, 0)
    cols = [
        jnp.broadcast_to(rows_lead[:, start + i : start + i + 1], shape) for i in range(MICRO)
    ]
    for i in range(MICRO):
        inv = lax.rsqrt(cols[i][i : i + 1, :])
        mult = cols[i] * inv
        for m in range(i + 1, MICRO):
            cols[m] = cols[m] - mult * mult[m : m + 1, :]
        below = jnp.where(row_ids > i, mult, 0.0)
        here = row_ids == i
        lead = rows_lead[i : i + 1, :] * inv
        tail = rows_tail[i : i + 1, :] * inv
        rows_lead = jnp.where(here, lead, rows_lead - below * lead)
        rows_tail = jnp.where(here, tail, rows_tail - below * tail)
    return rows_lead, rows_tail


def factor_steps(work, panel, out, emit, *, count, size):
    tiles = size // TILE
    row_ids = lax.broadcasted_iota(jnp.int32, (TILE, TILE), 0)
    col_ids = lax.broadcasted_iota(jnp.int32, (TILE, TILE), 1)

    def step(k, carry):
        at = pl.multiple_of(k * TILE, TILE)
        for blk in range(count):
            panel[blk, :, :TILE] = work[blk, pl.ds(at, TILE), pl.ds(at, TILE)]
            panel[blk, :, TILE:] = jnp.where(row_ids == col_ids, 1.0, 0.0)
        for start in range(0, TILE, MICRO):
            end = start + MICRO
            for blk in range(count):
                lead, tail = panel_rows(
                    panel[blk, start:end, :TILE], panel[blk, start:end, TILE:], start
                )
                panel[blk, start:end, :TILE] = lead
                panel[blk, start:end, TILE:] = tail
                if end < TILE:
                    left = left_parts(lead, 0)
                    right = right_parts(jnp.concatenate([lead, tail], axis=1))
                    panel[blk, end:, :] = panel[blk, end:, :] - cross(left, right)[end:, :]
        for blk in range(count):
            lower = jnp.where(row_ids >= col_ids, panel[blk, :, :TILE].T, 0.0)
            out[blk, pl.ds(at, TILE), pl.ds(at, TILE)] = lower
        for c in range(tiles - 1):

            @pl.when(k == c)
            def _():
                lo, mid = c * TILE, (c + 1) * TILE
                for blk in range(count):
                    upper = jnp.dot(
                        left_parts(panel[blk, :, TILE:], 1),
                        right_parts(work[blk, lo:mid, mid:]),
                        preferred_element_type=jnp.float32,
                    )
                    lower = upper.T
                    out[blk, mid:, lo:mid] = lower
                    out[blk, lo:mid, mid:] = jnp.zeros_like(upper)
                    left = left_parts(lower, 1)
                    right = right_parts(upper)
                    rest = size - mid
                    for first in range(0, rest, 2 * TILE):
                        last = min(first + 2 * TILE, rest)
                        update = jnp.dot(
                            left[first:last], right[:, first:], preferred_element_type=jnp.float32
                        )
                        r = mid + first
                        work[blk, r : mid + last, r:] = work[blk, r : mid + last, r:] - update

        emit(k)
        return carry

    lax.fori_loop(0, tiles, step, 0)


def across(left, right):
    return lax.dot_general(
        left, right, (((1,), (1,)), ((), ())), preferred_element_type=jnp.float32
    )


def spread_body(points, targets, phase, freqs, phi, points_out, freqs_out, turns_out, projected,
                pbuf, tbuf, fbuf, fown, cbuf, flipped, turns, in_sem,
                psend, precv, tsend, trecv, fsend, frecv, csend, crecv, pass_sem,
                *, data_count, feat_count, scale):
    me = lax.axis_index("dp")
    here = lax.axis_index("feat")
    chips = data_count // 2
    chip, core = me // 2, me % 2
    rows = points.shape[0]
    depth, width = freqs.shape
    tile_width = freqs_out.shape[1]
    partner = chip * 2 + (1 - core)
    holder = me * tile_width // width
    offset = pl.multiple_of(me * tile_width % width, tile_width)
    pieces = cbuf.shape[0]
    piece = tile_width // pieces
    side_x = (here % 2 + holder % 2) % 2
    side_y = (here // 2 + holder // 2) % 2
    opposite = 3 - holder

    loads = [
        pltpu.make_async_copy(points, pbuf.at[me], in_sem.at[0]),
        pltpu.make_async_copy(targets, tbuf.at[me], in_sem.at[1]),
        pltpu.make_async_copy(phase, fbuf.at[here], in_sem.at[2]),
        pltpu.make_async_copy(freqs, fown, in_sem.at[3]),
    ]
    for copy in loads:
        copy.start()

    def remote(source, target, send, recv, dp, feat):
        return pltpu.make_async_remote_copy(
            src_ref=source, dst_ref=target, send_sem=send, recv_sem=recv,
            device_id={"dp": dp, "feat": feat}, device_id_type=pl.DeviceIdType.MESH)

    barrier = pltpu.get_barrier_semaphore()
    for step in range(1, data_count):
        pl.semaphore_signal(
            barrier, inc=1, device_id={"dp": lax.rem(me + step, data_count), "feat": here},
            device_id_type=pl.DeviceIdType.MESH)
    for step in range(1, feat_count):
        pl.semaphore_signal(
            barrier, inc=1, device_id={"dp": me, "feat": lax.rem(here + step, feat_count)},
            device_id_type=pl.DeviceIdType.MESH)
    pl.semaphore_wait(barrier, data_count + feat_count - 2)

    def peer(step):
        return lax.rem(chip + step, chips) * 2 + core

    def points_copy(slot, sem, dp):
        return remote(pbuf.at[slot], pbuf.at[slot], sem, precv.at[slot], dp, here)

    def targets_copy(slot, step):
        dp = lax.rem(me + step, data_count)
        return remote(tbuf.at[slot], tbuf.at[slot], tsend.at[step], trecv.at[slot], dp, here)

    def phase_copy(slot, step):
        feat = lax.rem(here + step, feat_count)
        return remote(fbuf.at[slot], fbuf.at[slot], fsend.at[step], frecv.at[slot], me, feat)

    def freqs_copy(q, way, feat):
        source = fown.at[:, pl.ds(offset + q * piece, piece)]
        return remote(source, cbuf.at[q], csend.at[way * pieces + q], crecv.at[q], me, feat)

    def freqs_pass(q, t):
        return remote(cbuf.at[q], cbuf.at[q], csend.at[t], crecv.at[q], me, opposite)

    order = [(t + 1) // 2 if t % 2 else chips - t // 2 for t in range(1, chips)]
    loads[0].wait()
    points_copy(me, psend.at[0], partner).start()
    for step in order:
        points_copy(me, psend.at[step], peer(step)).start()
    loads[1].wait()
    for step in range(1, data_count):
        targets_copy(me, step).start()
    loads[2].wait()
    for step in range(1, feat_count):
        phase_copy(here, step).start()
    loads[3].wait()
    near_x = (1 - holder % 2) + holder // 2 * 2
    near_y = holder % 2 + (1 - holder // 2) * 2
    sends = [(q, 0, near_x) for q in range(pieces)]
    sends += [((q + pieces // 2) % pieces, 1, near_y) for q in range(pieces)]
    half = pieces // 2

    @pl.when(here == holder)
    def _():
        for q, way, feat in sends:
            freqs_copy(q, way, feat).start()

    flipped[...] = fown[...].T
    for first in range(0, width, TILE):
        row = fbuf[here, :, first : first + TILE] * (0.5 / math.pi)
        turns[first : first + TILE, :] = jnp.broadcast_to(row, (TILE, TILE)).T
    projected[...] = jnp.zeros_like(projected)
    step_width = min(width, 1024)

    def compute(slot):
        at = pl.multiple_of(slot * rows, rows)
        block = pbuf[slot]
        points_out[pl.ds(at, rows), :] = block

        def part(j, carry):
            feats = pl.ds(pl.multiple_of(j * step_width, step_width), step_width)
            angle = across(flipped[feats, :], block) * (0.5 / math.pi)
            shift = turns[feats, :]
            value = wave(angle + jnp.concatenate([shift] * (rows // TILE), axis=1), scale)
            phi[feats, pl.ds(at, rows)] = value
            projected[:, feats] = projected[:, feats] + across(tbuf[slot], value)
            return carry

        lax.fori_loop(0, width // step_width, part, 0)

    def targets_wait(slot):
        remote(tbuf.at[slot], tbuf.at[slot], tsend.at[1], trecv.at[slot], partner, here).wait_recv()

    compute(me)
    points_copy(partner, psend.at[0], partner).wait_recv()
    targets_wait(partner)
    compute(partner)

    def arrive(t, carry):
        odd = t % 2
        step = odd * ((t + 1) // 2) + (1 - odd) * (chips - t // 2)
        source = lax.rem(chip + chips - step, chips)
        same = source * 2 + core
        other = source * 2 + (1 - core)
        points_copy(same, psend.at[0], partner).wait_recv()
        points_copy(same, pass_sem.at[t], partner).start()
        targets_wait(same)
        compute(same)
        points_copy(other, psend.at[0], partner).wait_recv()
        targets_wait(other)
        compute(other)

        @pl.when((side_x + side_y == 1) & (t >= chips - half))
        def _():
            q = side_y * half + t - (chips - half)
            freqs_pass(q, 0).wait_recv()
            freqs_pass(q, t - (chips - half)).start()

        return carry

    lax.fori_loop(1, chips, arrive, 0)

    for step in range(1, feat_count):
        slot = lax.rem(here + step, feat_count)
        phase_copy(slot, step).wait_recv()
    turns_out[...] = fbuf[...] * (0.5 / math.pi)

    @pl.when(here == holder)
    def _():
        freqs_out[...] = fown[:, pl.ds(offset, tile_width)]
        for q, way, feat in sends:
            freqs_copy(q, way, feat).wait_send()

    @pl.when(side_x + side_y == 1)
    def _():
        for t in range(half):
            freqs_pass((1 - side_y) * half + t, 0).wait_recv()
            freqs_pass(side_y * half + t, t).wait_send()

    @pl.when(side_x + side_y == 2)
    def _():
        for q in range(pieces):
            freqs_pass(q, 0).wait_recv()

    @pl.when(here != holder)
    def _():
        for q in range(pieces):
            freqs_out[:, q * piece : (q + 1) * piece] = cbuf[q]

    points_copy(me, psend.at[0], partner).wait_send()
    for step in order:
        points_copy(me, psend.at[step], peer(step)).wait_send()
    for step in range(1, data_count):
        targets_copy(me, step).wait_send()
    for step in range(1, feat_count):
        phase_copy(here, step).wait_send()
    for t in range(1, chips):
        points_copy(me, pass_sem.at[t], partner).wait_send()


def spread(points, targets, phase, freqs, tile_width, scale):
    data_count, feat_count = lax.axis_size("dp"), lax.axis_size("feat")
    rows, depth = points.shape
    width = freqs.shape[1]
    outs = targets.shape[0]
    vmem = pl.BlockSpec(memory_space=pltpu.VMEM)
    hbm = pl.BlockSpec(memory_space=pltpu.HBM)
    dma = pltpu.SemaphoreType.DMA
    pieces = 4
    return pl.pallas_call(
        functools.partial(spread_body, data_count=data_count, feat_count=feat_count, scale=scale),
        out_shape=(
            jax.ShapeDtypeStruct((width, rows * data_count), jnp.bfloat16),
            jax.ShapeDtypeStruct((rows * data_count, depth), jnp.bfloat16),
            jax.ShapeDtypeStruct((depth, tile_width), jnp.bfloat16),
            jax.ShapeDtypeStruct((feat_count, 1, width), jnp.float32),
            jax.ShapeDtypeStruct((outs, width), jnp.float32),
        ),
        in_specs=[hbm] * 4,
        out_specs=[vmem] * 5,
        scratch_shapes=[
            pltpu.VMEM((data_count, rows, depth), jnp.bfloat16),
            pltpu.VMEM((data_count, outs, rows), jnp.bfloat16),
            pltpu.VMEM((feat_count, 1, width), jnp.float32),
            pltpu.VMEM((depth, width), jnp.bfloat16),
            pltpu.VMEM((pieces, depth, tile_width // pieces), jnp.bfloat16),
            pltpu.VMEM((width, depth), jnp.bfloat16),
            pltpu.VMEM((width, TILE), jnp.float32),
            dma((4,)),
            dma((data_count // 2,)),
            dma((data_count,)),
            dma((data_count,)),
            dma((data_count,)),
            dma((feat_count,)),
            dma((feat_count,)),
            dma((2 * pieces,)),
            dma((pieces,)),
            dma((data_count // 2,)),
        ],
        compiler_params=pltpu.CompilerParams(
            collective_id=0, has_side_effects=True, vmem_limit_bytes=24 * MIB
        ),
        cost_estimate=pl.CostEstimate(
            flops=2 * rows * data_count * depth * width,
            bytes_accessed=2 * rows * data_count * width,
            transcendentals=0,
        ),
        name="spread",
    )(points, targets, phase[None, :], freqs)


def factor_body(phi, sums, ridge, out, projected, work, block_out, panel, out_sem,
                *, count, size):
    projected[...] = sums[...]
    for blk in range(count):
        base = blk * size
        for c in range(0, size, WIDE):
            mid = c + WIDE
            tile = across(phi[base : base + mid, :], phi[base + c : base + mid, :])
            work[blk, :mid, c:mid] = with_ridge(tile, ridge[:, base + c : base + mid], 0, c)

    def rows_out(blk, k):
        at = pl.ds(pl.multiple_of(k * TILE, TILE), TILE)
        return pltpu.make_async_copy(block_out.at[blk, at], out.at[blk, at], out_sem.at[blk])

    def emit(k):
        for blk in range(count):
            rows_out(blk, k).start()

    factor_steps(work, panel, block_out, emit, count=count, size=size)
    for blk in range(count):
        pltpu.make_async_copy(block_out.at[blk], out.at[blk], out_sem.at[blk]).wait()


def factor(phi, sums, ridge, size):
    width, rows = phi.shape
    count = width // size
    outs = sums.shape[0]
    vmem = pl.BlockSpec(memory_space=pltpu.VMEM)
    hbm = pl.BlockSpec(memory_space=pltpu.HBM)
    return pl.pallas_call(
        functools.partial(factor_body, count=count, size=size),
        out_shape=(
            jax.ShapeDtypeStruct((count, size, size), jnp.float32),
            jax.ShapeDtypeStruct((outs, width), jnp.float32),
        ),
        in_specs=[vmem] * 3,
        out_specs=(hbm, vmem),
        scratch_shapes=[
            pltpu.VMEM((count, size, size), jnp.float32),
            pltpu.VMEM((count, size, size), jnp.float32),
            pltpu.VMEM((count, TILE, 2 * TILE), jnp.float32),
            pltpu.SemaphoreType.DMA((count,)),
        ],
        compiler_params=pltpu.CompilerParams(vmem_limit_bytes=32 * MIB),
        cost_estimate=pl.CostEstimate(
            flops=30 * rows * width * size, bytes_accessed=8 * rows * width, transcendentals=0
        ),
        name="lower_factors",
    )(phi, sums, ridge)


def tile_body(phi, points, freqs, phase, ridge, start, out, cols_phi, ring, out_sem, *, scale):
    width, rows = phi.shape
    columns = freqs.shape[1]
    slots, tall, _ = ring.shape
    down, wide = width // tall, columns // WIDE
    chunk = rows // down

    def make(j, r):
        cols = pl.ds(pl.multiple_of(j * WIDE, WIDE), WIDE)
        at = pl.ds(pl.multiple_of(r * chunk, chunk), chunk)
        cols_phi[lax.rem(j, 2), at, :] = features(
            points[at, :], freqs[:, cols], phase[:, cols], scale
        )

    def store(j, r, slot):
        return pltpu.make_async_copy(
            ring.at[slot],
            out.at[pl.ds(pl.multiple_of(r * tall, tall), tall),
                   pl.ds(pl.multiple_of(j * WIDE, WIDE), WIDE)],
            out_sem.at[slot])

    def first(r, carry):
        make(0, r)
        return carry

    lax.fori_loop(0, down, first, 0)

    def one(it, carry):
        j, r = it // down, lax.rem(it, down)
        slot = lax.rem(it, slots)

        @pl.when(it >= slots)
        def _():
            store(j, r, slot).wait()

        cols = pl.ds(pl.multiple_of(j * WIDE, WIDE), WIDE)
        at = pl.ds(pl.multiple_of(r * tall, tall), tall)
        tile = jnp.dot(phi[at, :], cols_phi[lax.rem(j, 2)], preferred_element_type=jnp.float32)
        ring[slot] = with_ridge(tile, ridge[:, cols], r * tall, j * WIDE + start[0])
        make(lax.rem(j + 1, wide), r)
        store(j, r, slot).start()
        return carry

    total = down * wide
    lax.fori_loop(0, total, one, 0)
    for it in range(total - slots, total):
        store(it // down, it % down, it % slots).wait()


def gram_tile(phi, points, freqs, phase, ridge, start, scale):
    width, rows = phi.shape
    columns = freqs.shape[1]
    vmem = pl.BlockSpec(memory_space=pltpu.VMEM)
    slots = 3
    return pl.pallas_call(
        functools.partial(tile_body, scale=scale),
        out_shape=jax.ShapeDtypeStruct((width, columns), jnp.float32),
        in_specs=[vmem, vmem, vmem, vmem, vmem, pl.BlockSpec(memory_space=pltpu.SMEM)],
        out_specs=pl.BlockSpec(memory_space=pltpu.HBM),
        scratch_shapes=[
            pltpu.VMEM((2, rows, WIDE), jnp.bfloat16),
            pltpu.VMEM((slots, 2 * WIDE, WIDE), jnp.float32),
            pltpu.SemaphoreType.DMA((slots,)),
        ],
        compiler_params=pltpu.CompilerParams(vmem_limit_bytes=24 * MIB),
        cost_estimate=pl.CostEstimate(
            flops=2 * rows * width * columns, bytes_accessed=4 * width * columns, transcendentals=0
        ),
        name="gram_tile",
    )(phi, points, freqs, phase, ridge, start)


def near_shards(points, freqs, phase, ridge, targets):
    data_count, feat_count = lax.axis_size("dp"), lax.axis_size("feat")
    data_index, feat_index = lax.axis_index("dp"), lax.axis_index("feat")
    local_width = freqs.shape[1]
    tile_width = local_width * feat_count // data_count
    scale = math.sqrt(2.0 / (points.shape[0] * data_count))
    phi, points_all, col_freqs, turns, sums = spread(
        points, targets, phase, freqs, tile_width, scale
    )
    factors, projected = factor(phi, sums, ridge[None, :], FB)
    col_start = data_index * tile_width
    start = col_start - feat_index * local_width
    col_turns = lax.dynamic_slice_in_dim(turns.reshape(1, -1), col_start, tile_width, 1)
    col_ridge = lax.dynamic_slice_in_dim(ridge[None, :], start, tile_width, 1)
    gram = gram_tile(phi, points_all, col_freqs, col_turns, col_ridge, start[None], scale)
    return gram, projected, factors.reshape(local_width, FB)


def lower_body(source, out, work, panel, sem, *, count, size):
    copy = pltpu.make_async_copy(source, work, sem)
    copy.start()
    copy.wait()
    factor_steps(work, panel, out, lambda k: None, count=count, size=size)


def lower_factors(blocks):
    count, size, _ = blocks.shape
    return pl.pallas_call(
        functools.partial(lower_body, count=count, size=size),
        out_shape=jax.ShapeDtypeStruct(blocks.shape, jnp.float32),
        in_specs=[pl.BlockSpec(memory_space=pl.ANY)],
        out_specs=pl.BlockSpec(memory_space=pltpu.VMEM),
        scratch_shapes=[
            pltpu.VMEM(blocks.shape, jnp.float32),
            pltpu.VMEM((count, TILE, 2 * TILE), jnp.float32),
            pltpu.SemaphoreType.DMA,
        ],
        compiler_params=pltpu.CompilerParams(vmem_limit_bytes=48 * MIB),
        name="lower_factors",
    )(blocks)


def wide_shards(points, freqs, phase, ridge, targets):
    data_count = lax.axis_size("dp")
    feat_count = lax.axis_size("feat")
    feat_index = lax.axis_index("feat")
    data_index = lax.axis_index("dp")
    local_width = freqs.shape[1]
    total_width = local_width * feat_count
    tile_width = total_width // data_count
    window = max(local_width, FB)
    window_start = feat_index * local_width // window * window
    row_start = feat_index * local_width
    col_start = data_index * tile_width
    scale = math.sqrt(2.0 / (points.shape[0] * data_count))
    points_all = lax.all_gather(points, "dp", axis=0, tiled=True)
    targets_all = lax.all_gather(targets, "dp", axis=1, tiled=True)
    freqs_all = lax.all_gather(freqs, "feat", axis=1, tiled=True)
    turns = phase * (0.5 / math.pi)
    turns_all, ridge_all = lax.all_gather(jnp.stack([turns, ridge]), "feat", axis=1, tiled=True)

    def features_at(start, width):
        return features(
            points_all,
            lax.dynamic_slice_in_dim(freqs_all, start, width, 1),
            lax.dynamic_slice_in_dim(turns_all, start, width, 0),
            scale,
        )

    window_phi = features_at(window_start, window)
    row_phi = lax.dynamic_slice_in_dim(window_phi, row_start - window_start, local_width, 1)
    window_ridge = lax.dynamic_slice_in_dim(ridge_all, window_start, window, 0)
    blocks = []
    for first in range(0, window, FB):
        part = window_phi[:, first : first + FB]
        block_ridge = window_ridge[first : first + FB, None]
        blocks.append(with_ridge(cross(part, part), block_ridge, 0, 0))
    factors_all = lower_factors(jnp.stack(blocks)).reshape(window, FB)
    factor_rows = lax.dynamic_slice_in_dim(factors_all, row_start - window_start, local_width, 0)
    col_phi = features_at(col_start, tile_width)
    gram_part = with_ridge(cross(row_phi, col_phi), ridge[:, None], row_start, col_start)
    projected = jnp.dot(targets_all, row_phi, preferred_element_type=jnp.float32)
    return gram_part, projected, factor_rows


def shards(points, freqs, phase, ridge, targets):
    local_width = freqs.shape[1]
    data_count, feat_count = lax.axis_size("dp"), lax.axis_size("feat")
    tile_width = local_width * feat_count // data_count
    near = (
        local_width % FB == 0
        and local_width % tile_width == 0
        and tile_width % WIDE == 0
        and data_count % 2 == 0
        and feat_count == 4
    )
    return (near_shards if near else wide_shards)(points, freqs, phase, ridge, targets)


def solution(mesh):
    in_specs = (P("dp", None), P(None, "feat"), P("feat"), P("feat"), P(None, "dp"))
    out_specs = (P("feat", "dp"), P(None, "feat"), P("feat", None))
    return jax.shard_map(shards, mesh=mesh, in_specs=in_specs, out_specs=out_specs, check_vma=False)
```

```python
import functools
import math

import jax
import jax.numpy as jnp
from jax import lax
from jax.experimental import pallas as pl
from jax.experimental.pallas import tpu as pltpu
from jax.sharding import PartitionSpec as P

FB = 1024
TILE = 128
MICRO = 16
WIDE = 256
BAND = 32
SUBLANES = 8
HALF = TILE // 2
MIB = 1024 * 1024
COS_TURNS = (
    0.9999991998413438,
    -19.738978175861334,
    64.92858783993428,
    -85.27084362691367,
    58.786940763031694,
    -21.065429407523915,
)


def features(rows, freq_cols, phase_turns, scale):
    angle = jnp.dot(rows, freq_cols, preferred_element_type=jnp.float32)
    return wave(angle * (0.5 / math.pi) + phase_turns, scale)


def wave(turns, scale):
    part = turns - jnp.round(turns)
    square = part * part
    poly = square * (scale * COS_TURNS[-1]) + scale * COS_TURNS[-2]
    for coeff in COS_TURNS[-3::-1]:
        poly = poly * square + scale * coeff
    return poly.astype(jnp.bfloat16)


def cross(left, right):
    return lax.dot_general(
        left, right, (((0,), (0,)), ((), ())), preferred_element_type=jnp.float32
    )


def with_ridge(tile, ridge, row_start, col_start):
    rows_here = row_start + lax.broadcasted_iota(jnp.int32, tile.shape, 0)
    cols_here = col_start + lax.broadcasted_iota(jnp.int32, tile.shape, 1)
    return tile + jnp.where(rows_here == cols_here, ridge, 0.0)


def halves(value):
    high = value.astype(jnp.bfloat16)
    return high, (value - high.astype(jnp.float32)).astype(jnp.bfloat16)


def left_parts(value, axis):
    high, low = halves(value)
    return jnp.concatenate([high, high, low], axis=axis)


def right_parts(value):
    high, low = halves(value)
    return jnp.concatenate([high, low, high], axis=0)


def panel_rows(rows_lead, rows_tail, start):
    shape = rows_lead.shape
    row_ids = lax.broadcasted_iota(jnp.int32, shape, 0)
    cols = [
        jnp.broadcast_to(rows_lead[:, start + i : start + i + 1], shape) for i in range(MICRO)
    ]
    for i in range(MICRO):
        inv = lax.rsqrt(cols[i][i : i + 1, :])
        mult = cols[i] * inv
        for m in range(i + 1, MICRO):
            cols[m] = cols[m] - mult * mult[m : m + 1, :]
        below = jnp.where(row_ids > i, mult, 0.0)
        here = row_ids == i
        lead = rows_lead[i : i + 1, :] * inv
        tail = rows_tail[i : i + 1, :] * inv
        rows_lead = jnp.where(here, lead, rows_lead - below * lead)
        rows_tail = jnp.where(here, tail, rows_tail - below * tail)
    return rows_lead, rows_tail


def spread_row(value, row):
    return jnp.broadcast_to(value[row : row + 1, :], value.shape)


def pair_rows(groups, own, base):
    shape = (SUBLANES, TILE)
    row_ids = lax.broadcasted_iota(jnp.int32, shape, 0)
    lanes = lax.broadcasted_iota(jnp.int32, shape, 1)
    side = jnp.where(lanes < HALF, base, base + HALF)
    count = len(groups)
    size = count * SUBLANES
    cols = [
        {
            g: jnp.take_along_axis(groups[g][own], side + m, axis=1)
            for g in range(m // SUBLANES, count)
        }
        for m in range(size)
    ]
    pivot = spread_row(cols[0][0], 0)
    for i in range(size):
        gi, ri = divmod(i, SUBLANES)
        inv = lax.rsqrt(pivot)
        if i + 1 < size:
            gn, rn = divmod(i + 1, SUBLANES)
            step = spread_row(cols[i][gn], rn) * inv
            pivot = spread_row(cols[i + 1][gn], rn) - step * step
        mult = {g: cols[i][g] * inv for g in range(gi, count)}
        for m in range(i + 1, size):
            gm, rm = divmod(m, SUBLANES)
            scalar = spread_row(mult[gm], rm)
            for g in range(gm, count):
                cols[m][g] = cols[m][g] - mult[g] * scalar
        below = jnp.where(row_ids > ri, mult[gi], 0.0)
        here = row_ids == ri
        for x in range(len(groups[0])):
            lead = spread_row(groups[gi][x], ri) * inv
            groups[gi][x] = jnp.where(here, lead, groups[gi][x] - below * lead)
            for g in range(gi + 1, count):
                groups[g][x] = groups[g][x] - mult[g] * lead
    return groups


def pair_panel(panel, beside):
    low = lax.broadcasted_iota(jnp.int32, (HALF, TILE), 1) < HALF
    for start in range(0, TILE, BAND):
        end = start + BAND
        beside(start // BAND)
        quarter = start // HALF
        parts = range(quarter, quarter + 3)
        groups = [
            [panel[x, r : r + SUBLANES, :] for x in parts]
            for r in range(start, end, SUBLANES)
        ]
        groups = pair_rows(groups, 0, start % HALF)
        for g, group in enumerate(groups):
            for x, value in zip(parts, group):
                panel[x, start + g * SUBLANES : start + (g + 1) * SUBLANES, :] = value
        bands = [jnp.concatenate([group[x] for group in groups], axis=0) for x in range(3)]
        right = right_parts(jnp.concatenate(bands, axis=1))
        for q in range(end // HALF, TILE // HALF):
            first = max(end - q * HALF, 0)
            update = cross(left_parts(bands[q - quarter], 0), right)
            for x in parts:
                at = (x - quarter) * TILE
                piece = jnp.where(
                    low[first:],
                    update[first:HALF, at : at + TILE],
                    update[HALF + first :, at : at + TILE],
                )
                rows = slice(q * HALF + first, (q + 1) * HALF)
                panel[x, rows, :] = panel[x, rows, :] - piece


def pair_steps(work, packed, panel, out, begin, beside, emit, *, size):
    tiles = size // TILE
    row_ids = lax.broadcasted_iota(jnp.int32, (TILE, TILE), 0)
    col_ids = lax.broadcasted_iota(jnp.int32, (TILE, TILE), 1)
    low = col_ids < HALF

    def swap(left, right):
        return (
            jnp.where(low, left, pltpu.roll(right, HALF, 1)),
            jnp.where(low, pltpu.roll(left, HALF, 1), right),
        )

    def step(k, carry):
        begin(k)
        at = pl.multiple_of(k * TILE, TILE)
        diagonal = [work[blk, pl.ds(at, TILE), pl.ds(at, TILE)] for blk in range(2)]
        packed[0], packed[1] = swap(*diagonal)
        packed[2] = jnp.where(row_ids == lax.rem(col_ids, HALF), 1.0, 0.0)
        packed[3] = jnp.where(row_ids == lax.rem(col_ids, HALF) + HALF, 1.0, 0.0)
        pair_panel(packed, functools.partial(beside, k))
        lead = swap(packed[0], packed[1])
        tail = swap(packed[2], packed[3])
        for blk in range(2):
            panel[blk] = tail[blk]
            lower = jnp.where(row_ids >= col_ids, lead[blk].T, 0.0)
            out[blk, pl.ds(at, TILE), pl.ds(at, TILE)] = lower
        for c in range(tiles - 1):

            @pl.when(k == c)
            def _():
                trailing(work, panel, out, c, 2, size)

        emit(k)
        return carry

    lax.fori_loop(0, tiles, step, 0)


def trailing(work, panel, out, c, count, size):
    lo, mid = c * TILE, (c + 1) * TILE
    for blk in range(count):
        upper = jnp.dot(
            left_parts(panel[blk], 1),
            right_parts(work[blk, lo:mid, mid:]),
            preferred_element_type=jnp.float32,
        )
        lower = upper.T
        out[blk, mid:, lo:mid] = lower
        out[blk, lo:mid, mid:] = jnp.zeros_like(upper)
        left = left_parts(lower, 1)
        right = right_parts(upper)
        rest = size - mid
        for first in range(0, rest, 2 * TILE):
            last = min(first + 2 * TILE, rest)
            update = jnp.dot(
                left[first:last], right[:, first:], preferred_element_type=jnp.float32
            )
            r = mid + first
            work[blk, r : mid + last, r:] = work[blk, r : mid + last, r:] - update


def factor_steps(work, panel, out, emit, *, count, size):
    tiles = size // TILE
    row_ids = lax.broadcasted_iota(jnp.int32, (TILE, TILE), 0)
    col_ids = lax.broadcasted_iota(jnp.int32, (TILE, TILE), 1)

    def step(k, carry):
        at = pl.multiple_of(k * TILE, TILE)
        for blk in range(count):
            panel[blk, :, :TILE] = work[blk, pl.ds(at, TILE), pl.ds(at, TILE)]
            panel[blk, :, TILE:] = jnp.where(row_ids == col_ids, 1.0, 0.0)
        for start in range(0, TILE, MICRO):
            end = start + MICRO
            for blk in range(count):
                lead, tail = panel_rows(
                    panel[blk, start:end, :TILE], panel[blk, start:end, TILE:], start
                )
                panel[blk, start:end, :TILE] = lead
                panel[blk, start:end, TILE:] = tail
                if end < TILE:
                    left = left_parts(lead, 0)
                    right = right_parts(jnp.concatenate([lead, tail], axis=1))
                    panel[blk, end:, :] = panel[blk, end:, :] - cross(left, right)[end:, :]
        for blk in range(count):
            lower = jnp.where(row_ids >= col_ids, panel[blk, :, :TILE].T, 0.0)
            out[blk, pl.ds(at, TILE), pl.ds(at, TILE)] = lower
        for c in range(tiles - 1):

            @pl.when(k == c)
            def _():
                lo, mid = c * TILE, (c + 1) * TILE
                for blk in range(count):
                    upper = jnp.dot(
                        left_parts(panel[blk, :, TILE:], 1),
                        right_parts(work[blk, lo:mid, mid:]),
                        preferred_element_type=jnp.float32,
                    )
                    lower = upper.T
                    out[blk, mid:, lo:mid] = lower
                    out[blk, lo:mid, mid:] = jnp.zeros_like(upper)
                    left = left_parts(lower, 1)
                    right = right_parts(upper)
                    rest = size - mid
                    for first in range(0, rest, 2 * TILE):
                        last = min(first + 2 * TILE, rest)
                        update = jnp.dot(
                            left[first:last], right[:, first:], preferred_element_type=jnp.float32
                        )
                        r = mid + first
                        work[blk, r : mid + last, r:] = work[blk, r : mid + last, r:] - update

        emit(k)
        return carry

    lax.fori_loop(0, tiles, step, 0)


def across(left, right):
    return lax.dot_general(
        left, right, (((1,), (1,)), ((), ())), preferred_element_type=jnp.float32
    )


def spread_body(points, targets, phase, freqs, phi, points_out, freqs_out, turns_out, projected,
                pbuf, tbuf, fbuf, fown, cbuf, flipped, turns, in_sem,
                psend, precv, tsend, trecv, fsend, frecv, csend, crecv, pass_sem,
                *, data_count, feat_count, scale):
    me = lax.axis_index("dp")
    here = lax.axis_index("feat")
    chips = data_count // 2
    chip, core = me // 2, me % 2
    rows = points.shape[0]
    depth, width = freqs.shape
    tile_width = freqs_out.shape[1]
    partner = chip * 2 + (1 - core)
    holder = me * tile_width // width
    offset = pl.multiple_of(me * tile_width % width, tile_width)
    pieces = cbuf.shape[0]
    piece = tile_width // pieces
    side_x = (here % 2 + holder % 2) % 2
    side_y = (here // 2 + holder // 2) % 2
    opposite = 3 - holder

    loads = [
        pltpu.make_async_copy(points, pbuf.at[me], in_sem.at[0]),
        pltpu.make_async_copy(targets, tbuf.at[me], in_sem.at[1]),
        pltpu.make_async_copy(phase, fbuf.at[here], in_sem.at[2]),
        pltpu.make_async_copy(freqs, fown, in_sem.at[3]),
    ]
    for copy in loads:
        copy.start()

    def remote(source, target, send, recv, dp, feat):
        return pltpu.make_async_remote_copy(
            src_ref=source, dst_ref=target, send_sem=send, recv_sem=recv,
            device_id={"dp": dp, "feat": feat}, device_id_type=pl.DeviceIdType.MESH)

    barrier = pltpu.get_barrier_semaphore()
    for step in range(1, data_count):
        pl.semaphore_signal(
            barrier, inc=1, device_id={"dp": lax.rem(me + step, data_count), "feat": here},
            device_id_type=pl.DeviceIdType.MESH)
    for step in range(1, feat_count):
        pl.semaphore_signal(
            barrier, inc=1, device_id={"dp": me, "feat": lax.rem(here + step, feat_count)},
            device_id_type=pl.DeviceIdType.MESH)
    pl.semaphore_wait(barrier, data_count + feat_count - 2)

    def peer(step):
        return lax.rem(chip + step, chips) * 2 + core

    def points_copy(slot, sem, dp):
        return remote(pbuf.at[slot], pbuf.at[slot], sem, precv.at[slot], dp, here)

    def targets_copy(slot, step):
        dp = lax.rem(me + step, data_count)
        return remote(tbuf.at[slot], tbuf.at[slot], tsend.at[step], trecv.at[slot], dp, here)

    def phase_copy(slot, step):
        feat = lax.rem(here + step, feat_count)
        return remote(fbuf.at[slot], fbuf.at[slot], fsend.at[step], frecv.at[slot], me, feat)

    def freqs_copy(q, way, feat):
        source = fown.at[:, pl.ds(offset + q * piece, piece)]
        return remote(source, cbuf.at[q], csend.at[way * pieces + q], crecv.at[q], me, feat)

    def freqs_pass(q, t):
        return remote(cbuf.at[q], cbuf.at[q], csend.at[t], crecv.at[q], me, opposite)

    order = [(t + 1) // 2 if t % 2 else chips - t // 2 for t in range(1, chips)]
    loads[0].wait()
    points_copy(me, psend.at[0], partner).start()
    for step in order:
        points_copy(me, psend.at[step], peer(step)).start()
    loads[1].wait()
    for step in range(1, data_count):
        targets_copy(me, step).start()
    loads[2].wait()
    for step in range(1, feat_count):
        phase_copy(here, step).start()
    loads[3].wait()
    near_x = (1 - holder % 2) + holder // 2 * 2
    near_y = holder % 2 + (1 - holder // 2) * 2
    sends = [(q, 0, near_x) for q in range(pieces)]
    sends += [((q + pieces // 2) % pieces, 1, near_y) for q in range(pieces)]
    half = pieces // 2

    @pl.when(here == holder)
    def _():
        for q, way, feat in sends:
            freqs_copy(q, way, feat).start()

    flipped[...] = fown[...].T
    for first in range(0, width, TILE):
        row = fbuf[here, :, first : first + TILE] * (0.5 / math.pi)
        turns[first : first + TILE, :] = jnp.broadcast_to(row, (TILE, TILE)).T
    projected[...] = jnp.zeros_like(projected)
    step_width = min(width, 1024)

    def compute(slot):
        at = pl.multiple_of(slot * rows, rows)
        block = pbuf[slot]
        points_out[pl.ds(at, rows), :] = block

        def part(j, carry):
            feats = pl.ds(pl.multiple_of(j * step_width, step_width), step_width)
            angle = across(flipped[feats, :], block) * (0.5 / math.pi)
            shift = turns[feats, :]
            value = wave(angle + jnp.concatenate([shift] * (rows // TILE), axis=1), scale)
            phi[feats, pl.ds(at, rows)] = value
            projected[:, feats] = projected[:, feats] + across(tbuf[slot], value)
            return carry

        lax.fori_loop(0, width // step_width, part, 0)

    def targets_wait(slot):
        remote(tbuf.at[slot], tbuf.at[slot], tsend.at[1], trecv.at[slot], partner, here).wait_recv()

    compute(me)
    points_copy(partner, psend.at[0], partner).wait_recv()
    targets_wait(partner)
    compute(partner)

    def arrive(t, carry):
        odd = t % 2
        step = odd * ((t + 1) // 2) + (1 - odd) * (chips - t // 2)
        source = lax.rem(chip + chips - step, chips)
        same = source * 2 + core
        other = source * 2 + (1 - core)
        points_copy(same, psend.at[0], partner).wait_recv()
        points_copy(same, pass_sem.at[t], partner).start()
        targets_wait(same)
        compute(same)
        points_copy(other, psend.at[0], partner).wait_recv()
        targets_wait(other)
        compute(other)

        @pl.when((side_x + side_y == 1) & (t <= half))
        def _():
            q = side_y * half + t - 1
            freqs_pass(q, 0).wait_recv()
            freqs_pass(q, t - 1).start()

        return carry

    lax.fori_loop(1, chips, arrive, 0)

    for step in range(1, feat_count):
        slot = lax.rem(here + step, feat_count)
        phase_copy(slot, step).wait_recv()
    turns_out[...] = fbuf[...] * (0.5 / math.pi)

    @pl.when(here == holder)
    def _():
        freqs_out[...] = fown[:, pl.ds(offset, tile_width)]
        for q, way, feat in sends:
            freqs_copy(q, way, feat).wait_send()

    @pl.when(side_x + side_y == 1)
    def _():
        for t in range(half):
            freqs_pass((1 - side_y) * half + t, 0).wait_recv()
            freqs_pass(side_y * half + t, t).wait_send()

    @pl.when(side_x + side_y == 2)
    def _():
        for q in range(pieces):
            freqs_pass(q, 0).wait_recv()

    @pl.when(here != holder)
    def _():
        for q in range(pieces):
            freqs_out[:, q * piece : (q + 1) * piece] = cbuf[q]

    points_copy(me, psend.at[0], partner).wait_send()
    for step in order:
        points_copy(me, psend.at[step], peer(step)).wait_send()
    for step in range(1, data_count):
        targets_copy(me, step).wait_send()
    for step in range(1, feat_count):
        phase_copy(here, step).wait_send()
    for t in range(1, chips):
        points_copy(me, pass_sem.at[t], partner).wait_send()


def spread(points, targets, phase, freqs, tile_width, scale):
    data_count, feat_count = lax.axis_size("dp"), lax.axis_size("feat")
    rows, depth = points.shape
    width = freqs.shape[1]
    outs = targets.shape[0]
    vmem = pl.BlockSpec(memory_space=pltpu.VMEM)
    hbm = pl.BlockSpec(memory_space=pltpu.HBM)
    dma = pltpu.SemaphoreType.DMA
    pieces = 4
    return pl.pallas_call(
        functools.partial(spread_body, data_count=data_count, feat_count=feat_count, scale=scale),
        out_shape=(
            jax.ShapeDtypeStruct((width, rows * data_count), jnp.bfloat16),
            jax.ShapeDtypeStruct((rows * data_count, depth), jnp.bfloat16),
            jax.ShapeDtypeStruct((depth, tile_width), jnp.bfloat16),
            jax.ShapeDtypeStruct((feat_count, 1, width), jnp.float32),
            jax.ShapeDtypeStruct((outs, width), jnp.float32),
        ),
        in_specs=[hbm] * 4,
        out_specs=[vmem] * 5,
        scratch_shapes=[
            pltpu.VMEM((data_count, rows, depth), jnp.bfloat16),
            pltpu.VMEM((data_count, outs, rows), jnp.bfloat16),
            pltpu.VMEM((feat_count, 1, width), jnp.float32),
            pltpu.VMEM((depth, width), jnp.bfloat16),
            pltpu.VMEM((pieces, depth, tile_width // pieces), jnp.bfloat16),
            pltpu.VMEM((width, depth), jnp.bfloat16),
            pltpu.VMEM((width, TILE), jnp.float32),
            dma((4,)),
            dma((data_count // 2,)),
            dma((data_count,)),
            dma((data_count,)),
            dma((data_count,)),
            dma((feat_count,)),
            dma((feat_count,)),
            dma((2 * pieces,)),
            dma((pieces,)),
            dma((data_count // 2,)),
        ],
        compiler_params=pltpu.CompilerParams(
            collective_id=0, has_side_effects=True, vmem_limit_bytes=24 * MIB
        ),
        cost_estimate=pl.CostEstimate(
            flops=2 * rows * data_count * depth * width,
            bytes_accessed=2 * rows * data_count * width,
            transcendentals=0,
        ),
        name="spread",
    )(points, targets, phase[None, :], freqs)


def assemble_body(phi, sums, ridge, points, freqs, phase, col_ridge, start, out, projected, gram,
                  work, block_out, packed, panel, cols_phi, ring, out_sem, ring_sem,
                  *, count, size, scale):
    projected[...] = sums[...]
    width, rows = phi.shape
    columns = freqs.shape[1]
    bands = TILE // BAND
    wide, down = columns // WIDE, width // WIDE
    parts = down // bands
    chunk = rows // down
    tall = bands * WIDE

    def make(j, r):
        cols = pl.ds(pl.multiple_of(j * WIDE, WIDE), WIDE)
        at = pl.ds(pl.multiple_of(r * chunk, chunk), chunk)
        cols_phi[lax.rem(j, 2), at, :] = features(
            points[at, :], freqs[:, cols], phase[:, cols], scale
        )

    def first(r, carry):
        make(0, r)
        return carry

    lax.fori_loop(0, down, first, 0)
    for blk in range(count):
        base = blk * size
        for c in range(0, size, WIDE):
            mid = c + WIDE
            tile = across(phi[base : base + mid, :], phi[base + c : base + mid, :])
            work[blk, :mid, c:mid] = with_ridge(tile, ridge[:, base + c : base + mid], 0, c)

    def rows_out(blk, k):
        at = pl.ds(pl.multiple_of(k * TILE, TILE), TILE)
        return pltpu.make_async_copy(block_out.at[blk, at], out.at[blk, at], out_sem.at[blk])

    def place(k):
        return k // parts, lax.rem(k, parts)

    def ring_out(k):
        j, part = place(k)
        slot = lax.rem(k, 2)
        return pltpu.make_async_copy(
            ring.at[slot],
            gram.at[pl.ds(pl.multiple_of(part * tall, tall), tall),
                    pl.ds(pl.multiple_of(j * WIDE, WIDE), WIDE)],
            ring_sem.at[slot])

    def begin(k):
        @pl.when(k >= 2)
        def _():
            ring_out(k).wait()

    def beside(k, band):
        j, part = place(k)
        r = part * bands + band
        at = pl.ds(pl.multiple_of(r * WIDE, WIDE), WIDE)
        ring[lax.rem(k, 2), band * WIDE : (band + 1) * WIDE, :] = jnp.dot(
            phi[at, :], cols_phi[lax.rem(j, 2)], preferred_element_type=jnp.float32
        )
        make(lax.rem(j + 1, wide), r)

    def emit(k):
        j, part = place(k)
        shift = start[0] + j * WIDE - part * tall

        @pl.when((shift >= 0) & (shift < tall))
        def _():
            at = pl.ds(pl.multiple_of(shift, WIDE), WIDE)
            cols = pl.ds(pl.multiple_of(j * WIDE, WIDE), WIDE)
            slot = lax.rem(k, 2)
            ring[slot, at, :] = with_ridge(ring[slot, at, :], col_ridge[:, cols], 0, 0)

        ring_out(k).start()
        for blk in range(count):
            rows_out(blk, k).start()

    pair_steps(work, packed, panel, block_out, begin, beside, emit, size=size)
    tiles = size // TILE
    for k in range(tiles - 2, tiles):
        ring_out(k).wait()
    for blk in range(count):
        pltpu.make_async_copy(block_out.at[blk], out.at[blk], out_sem.at[blk]).wait()


def assemble(phi, sums, ridge, points, freqs, phase, col_ridge, start, size, scale):
    width, rows = phi.shape
    columns = freqs.shape[1]
    count = width // size
    outs = sums.shape[0]
    vmem = pl.BlockSpec(memory_space=pltpu.VMEM)
    hbm = pl.BlockSpec(memory_space=pltpu.HBM)
    return pl.pallas_call(
        functools.partial(assemble_body, count=count, size=size, scale=scale),
        out_shape=(
            jax.ShapeDtypeStruct((count, size, size), jnp.float32),
            jax.ShapeDtypeStruct((outs, width), jnp.float32),
            jax.ShapeDtypeStruct((width, columns), jnp.float32),
        ),
        in_specs=[vmem] * 7 + [pl.BlockSpec(memory_space=pltpu.SMEM)],
        out_specs=(hbm, vmem, hbm),
        scratch_shapes=[
            pltpu.VMEM((count, size, size), jnp.float32),
            pltpu.VMEM((count, size, size), jnp.float32),
            pltpu.VMEM((4, TILE, TILE), jnp.float32),
            pltpu.VMEM((count, TILE, TILE), jnp.float32),
            pltpu.VMEM((2, rows, WIDE), jnp.bfloat16),
            pltpu.VMEM((2, TILE // BAND * WIDE, WIDE), jnp.float32),
            pltpu.SemaphoreType.DMA((count,)),
            pltpu.SemaphoreType.DMA((2,)),
        ],
        compiler_params=pltpu.CompilerParams(vmem_limit_bytes=40 * MIB),
        cost_estimate=pl.CostEstimate(
            flops=30 * rows * width * size, bytes_accessed=8 * rows * width, transcendentals=0
        ),
        name="assemble",
    )(phi, sums, ridge, points, freqs, phase, col_ridge, start)


def near_shards(points, freqs, phase, ridge, targets):
    data_count, feat_count = lax.axis_size("dp"), lax.axis_size("feat")
    data_index, feat_index = lax.axis_index("dp"), lax.axis_index("feat")
    local_width = freqs.shape[1]
    tile_width = local_width * feat_count // data_count
    scale = math.sqrt(2.0 / (points.shape[0] * data_count))
    phi, points_all, col_freqs, turns, sums = spread(
        points, targets, phase, freqs, tile_width, scale
    )
    col_start = data_index * tile_width
    start = col_start - feat_index * local_width
    col_turns = lax.dynamic_slice_in_dim(turns.reshape(1, -1), col_start, tile_width, 1)
    col_ridge = lax.dynamic_slice_in_dim(ridge[None, :], start, tile_width, 1)
    factors, projected, gram = assemble(
        phi, sums, ridge[None, :], points_all, col_freqs, col_turns, col_ridge, start[None],
        FB, scale,
    )
    return gram, projected, factors.reshape(local_width, FB)


def lower_body(source, out, work, panel, sem, *, count, size):
    copy = pltpu.make_async_copy(source, work, sem)
    copy.start()
    copy.wait()
    factor_steps(work, panel, out, lambda k: None, count=count, size=size)


def lower_factors(blocks):
    count, size, _ = blocks.shape
    return pl.pallas_call(
        functools.partial(lower_body, count=count, size=size),
        out_shape=jax.ShapeDtypeStruct(blocks.shape, jnp.float32),
        in_specs=[pl.BlockSpec(memory_space=pl.ANY)],
        out_specs=pl.BlockSpec(memory_space=pltpu.VMEM),
        scratch_shapes=[
            pltpu.VMEM(blocks.shape, jnp.float32),
            pltpu.VMEM((count, TILE, 2 * TILE), jnp.float32),
            pltpu.SemaphoreType.DMA,
        ],
        compiler_params=pltpu.CompilerParams(vmem_limit_bytes=48 * MIB),
        name="lower_factors",
    )(blocks)


def wide_shards(points, freqs, phase, ridge, targets):
    data_count = lax.axis_size("dp")
    feat_count = lax.axis_size("feat")
    feat_index = lax.axis_index("feat")
    data_index = lax.axis_index("dp")
    local_width = freqs.shape[1]
    total_width = local_width * feat_count
    tile_width = total_width // data_count
    window = max(local_width, FB)
    window_start = feat_index * local_width // window * window
    row_start = feat_index * local_width
    col_start = data_index * tile_width
    scale = math.sqrt(2.0 / (points.shape[0] * data_count))
    points_all = lax.all_gather(points, "dp", axis=0, tiled=True)
    targets_all = lax.all_gather(targets, "dp", axis=1, tiled=True)
    freqs_all = lax.all_gather(freqs, "feat", axis=1, tiled=True)
    turns = phase * (0.5 / math.pi)
    turns_all, ridge_all = lax.all_gather(jnp.stack([turns, ridge]), "feat", axis=1, tiled=True)

    def features_at(start, width):
        return features(
            points_all,
            lax.dynamic_slice_in_dim(freqs_all, start, width, 1),
            lax.dynamic_slice_in_dim(turns_all, start, width, 0),
            scale,
        )

    window_phi = features_at(window_start, window)
    row_phi = lax.dynamic_slice_in_dim(window_phi, row_start - window_start, local_width, 1)
    window_ridge = lax.dynamic_slice_in_dim(ridge_all, window_start, window, 0)
    blocks = []
    for first in range(0, window, FB):
        part = window_phi[:, first : first + FB]
        block_ridge = window_ridge[first : first + FB, None]
        blocks.append(with_ridge(cross(part, part), block_ridge, 0, 0))
    factors_all = lower_factors(jnp.stack(blocks)).reshape(window, FB)
    factor_rows = lax.dynamic_slice_in_dim(factors_all, row_start - window_start, local_width, 0)
    col_phi = features_at(col_start, tile_width)
    gram_part = with_ridge(cross(row_phi, col_phi), ridge[:, None], row_start, col_start)
    projected = jnp.dot(targets_all, row_phi, preferred_element_type=jnp.float32)
    return gram_part, projected, factor_rows


def shards(points, freqs, phase, ridge, targets):
    local_width = freqs.shape[1]
    data_count, feat_count = lax.axis_size("dp"), lax.axis_size("feat")
    tile_width = local_width * feat_count // data_count
    near = (
        local_width == 2 * FB
        and local_width % tile_width == 0
        and tile_width % WIDE == 0
        and tile_width // WIDE * (local_width // WIDE) == FB // BAND
        and points.shape[0] * data_count % (local_width // WIDE) == 0
        and data_count % 2 == 0
        and feat_count == 4
    )
    return (near_shards if near else wide_shards)(points, freqs, phase, ridge, targets)


def solution(mesh):
    in_specs = (P("dp", None), P(None, "feat"), P("feat"), P("feat"), P(None, "dp"))
    out_specs = (P("feat", "dp"), P(None, "feat"), P("feat", None))
    return jax.shard_map(shards, mesh=mesh, in_specs=in_specs, out_specs=out_specs, check_vma=False)
```

```python
import functools
import math

import jax
import jax.numpy as jnp
from jax import lax
from jax.experimental import pallas as pl
from jax.experimental.pallas import tpu as pltpu
from jax.sharding import PartitionSpec as P

FB = 1024
TILE = 128
MICRO = 16
WIDE = 256
BAND = 32
SUBBAND = 16
SUBLANES = 8
HALF = TILE // 2
MIB = 1024 * 1024
COS_TURNS = (
    0.9999991998413438,
    -19.738978175861334,
    64.92858783993428,
    -85.27084362691367,
    58.786940763031694,
    -21.065429407523915,
)


def features(rows, freq_cols, phase_turns, scale):
    angle = jnp.dot(rows, freq_cols, preferred_element_type=jnp.float32)
    return wave(angle * (0.5 / math.pi) + phase_turns, scale)


def wave(turns, scale):
    part = turns - jnp.round(turns)
    square = part * part
    poly = square * (scale * COS_TURNS[-1]) + scale * COS_TURNS[-2]
    for coeff in COS_TURNS[-3::-1]:
        poly = poly * square + scale * coeff
    return poly.astype(jnp.bfloat16)


def cross(left, right):
    return lax.dot_general(
        left, right, (((0,), (0,)), ((), ())), preferred_element_type=jnp.float32
    )


def with_ridge(tile, ridge, row_start, col_start):
    rows_here = row_start + lax.broadcasted_iota(jnp.int32, tile.shape, 0)
    cols_here = col_start + lax.broadcasted_iota(jnp.int32, tile.shape, 1)
    return tile + jnp.where(rows_here == cols_here, ridge, 0.0)


def halves(value):
    high = value.astype(jnp.bfloat16)
    return high, (value - high.astype(jnp.float32)).astype(jnp.bfloat16)


def left_parts(value, axis):
    high, low = halves(value)
    return jnp.concatenate([high, high, low], axis=axis)


def right_parts(value):
    high, low = halves(value)
    return jnp.concatenate([high, low, high], axis=0)


def panel_rows(rows_lead, rows_tail, start):
    shape = rows_lead.shape
    row_ids = lax.broadcasted_iota(jnp.int32, shape, 0)
    cols = [
        jnp.broadcast_to(rows_lead[:, start + i : start + i + 1], shape) for i in range(MICRO)
    ]
    for i in range(MICRO):
        inv = lax.rsqrt(cols[i][i : i + 1, :])
        mult = cols[i] * inv
        for m in range(i + 1, MICRO):
            cols[m] = cols[m] - mult * mult[m : m + 1, :]
        below = jnp.where(row_ids > i, mult, 0.0)
        here = row_ids == i
        lead = rows_lead[i : i + 1, :] * inv
        tail = rows_tail[i : i + 1, :] * inv
        rows_lead = jnp.where(here, lead, rows_lead - below * lead)
        rows_tail = jnp.where(here, tail, rows_tail - below * tail)
    return rows_lead, rows_tail


def spread_row(value, row):
    return jnp.broadcast_to(value[row : row + 1, :], value.shape)


def pair_rows(groups, own, base):
    shape = (SUBLANES, TILE)
    row_ids = lax.broadcasted_iota(jnp.int32, shape, 0)
    lanes = lax.broadcasted_iota(jnp.int32, shape, 1)
    side = jnp.where(lanes < HALF, base, base + HALF)
    count = len(groups)
    size = count * SUBLANES
    for first in range(0, size, SUBBAND):
        span = range(first, first + SUBBAND)
        cols = {
            m: {
                g: jnp.take_along_axis(groups[g][own], side + m, axis=1)
                for g in range(m // SUBLANES, count)
            }
            for m in span
        }
        pivot = spread_row(cols[first][first // SUBLANES], first % SUBLANES)
        for i in span:
            gi, ri = divmod(i, SUBLANES)
            inv = lax.rsqrt(pivot)
            if i + 1 in span:
                gn, rn = divmod(i + 1, SUBLANES)
                step = spread_row(cols[i][gn], rn) * inv
                pivot = spread_row(cols[i + 1][gn], rn) - step * step
            mult = {g: cols[i][g] * inv for g in range(gi, count)}
            for m in range(i + 1, span.stop):
                gm, rm = divmod(m, SUBLANES)
                scalar = spread_row(mult[gm], rm)
                for g in range(gm, count):
                    cols[m][g] = cols[m][g] - mult[g] * scalar
            below = jnp.where(row_ids > ri, mult[gi], 0.0)
            here = row_ids == ri
            for x in range(len(groups[0])):
                lead = spread_row(groups[gi][x], ri) * inv
                groups[gi][x] = jnp.where(here, lead, groups[gi][x] - below * lead)
                for g in range(gi + 1, count):
                    groups[g][x] = groups[g][x] - mult[g] * lead
    return groups


def pair_panel(panel, beside):
    low = lax.broadcasted_iota(jnp.int32, (HALF, TILE), 1) < HALF
    for start in range(0, TILE, BAND):
        end = start + BAND
        beside(start // BAND)
        quarter = start // HALF
        parts = range(quarter, quarter + 3)
        groups = [
            [panel[x, r : r + SUBLANES, :] for x in parts]
            for r in range(start, end, SUBLANES)
        ]
        groups = pair_rows(groups, 0, start % HALF)
        for g, group in enumerate(groups):
            for x, value in zip(parts, group):
                panel[x, start + g * SUBLANES : start + (g + 1) * SUBLANES, :] = value
        bands = [jnp.concatenate([group[x] for group in groups], axis=0) for x in range(3)]
        right = right_parts(jnp.concatenate(bands, axis=1))
        for q in range(end // HALF, TILE // HALF):
            first = max(end - q * HALF, 0)
            update = cross(left_parts(bands[q - quarter], 0), right)
            for x in parts:
                at = (x - quarter) * TILE
                piece = jnp.where(
                    low[first:],
                    update[first:HALF, at : at + TILE],
                    update[HALF + first :, at : at + TILE],
                )
                rows = slice(q * HALF + first, (q + 1) * HALF)
                panel[x, rows, :] = panel[x, rows, :] - piece


def pair_steps(work, packed, panel, out, begin, beside, emit, *, size):
    tiles = size // TILE
    row_ids = lax.broadcasted_iota(jnp.int32, (TILE, TILE), 0)
    col_ids = lax.broadcasted_iota(jnp.int32, (TILE, TILE), 1)
    low = col_ids < HALF

    def swap(left, right):
        return (
            jnp.where(low, left, pltpu.roll(right, HALF, 1)),
            jnp.where(low, pltpu.roll(left, HALF, 1), right),
        )

    def step(k, carry):
        begin(k)
        at = pl.multiple_of(k * TILE, TILE)
        diagonal = [work[blk, pl.ds(at, TILE), pl.ds(at, TILE)] for blk in range(2)]
        packed[0], packed[1] = swap(*diagonal)
        packed[2] = jnp.where(row_ids == lax.rem(col_ids, HALF), 1.0, 0.0)
        packed[3] = jnp.where(row_ids == lax.rem(col_ids, HALF) + HALF, 1.0, 0.0)
        pair_panel(packed, functools.partial(beside, k))
        lead = swap(packed[0], packed[1])
        tail = swap(packed[2], packed[3])
        for blk in range(2):
            panel[blk] = tail[blk]
            lower = jnp.where(row_ids >= col_ids, lead[blk].T, 0.0)
            out[blk, pl.ds(at, TILE), pl.ds(at, TILE)] = lower
        for c in range(tiles - 1):

            @pl.when(k == c)
            def _():
                trailing(work, panel, out, c, 2, size)

        emit(k)
        return carry

    lax.fori_loop(0, tiles, step, 0)


def trailing(work, panel, out, c, count, size):
    lo, mid = c * TILE, (c + 1) * TILE
    for blk in range(count):
        upper = jnp.dot(
            left_parts(panel[blk], 1),
            right_parts(work[blk, lo:mid, mid:]),
            preferred_element_type=jnp.float32,
        )
        lower = upper.T
        out[blk, mid:, lo:mid] = lower
        out[blk, lo:mid, mid:] = jnp.zeros_like(upper)
        left = left_parts(lower, 1)
        right = right_parts(upper)
        rest = size - mid
        for first in range(0, rest, 2 * TILE):
            last = min(first + 2 * TILE, rest)
            update = jnp.dot(
                left[first:last], right[:, first:], preferred_element_type=jnp.float32
            )
            r = mid + first
            work[blk, r : mid + last, r:] = work[blk, r : mid + last, r:] - update


def factor_steps(work, panel, out, emit, *, count, size):
    tiles = size // TILE
    row_ids = lax.broadcasted_iota(jnp.int32, (TILE, TILE), 0)
    col_ids = lax.broadcasted_iota(jnp.int32, (TILE, TILE), 1)

    def step(k, carry):
        at = pl.multiple_of(k * TILE, TILE)
        for blk in range(count):
            panel[blk, :, :TILE] = work[blk, pl.ds(at, TILE), pl.ds(at, TILE)]
            panel[blk, :, TILE:] = jnp.where(row_ids == col_ids, 1.0, 0.0)
        for start in range(0, TILE, MICRO):
            end = start + MICRO
            for blk in range(count):
                lead, tail = panel_rows(
                    panel[blk, start:end, :TILE], panel[blk, start:end, TILE:], start
                )
                panel[blk, start:end, :TILE] = lead
                panel[blk, start:end, TILE:] = tail
                if end < TILE:
                    left = left_parts(lead, 0)
                    right = right_parts(jnp.concatenate([lead, tail], axis=1))
                    panel[blk, end:, :] = panel[blk, end:, :] - cross(left, right)[end:, :]
        for blk in range(count):
            lower = jnp.where(row_ids >= col_ids, panel[blk, :, :TILE].T, 0.0)
            out[blk, pl.ds(at, TILE), pl.ds(at, TILE)] = lower
        for c in range(tiles - 1):

            @pl.when(k == c)
            def _():
                lo, mid = c * TILE, (c + 1) * TILE
                for blk in range(count):
                    upper = jnp.dot(
                        left_parts(panel[blk, :, TILE:], 1),
                        right_parts(work[blk, lo:mid, mid:]),
                        preferred_element_type=jnp.float32,
                    )
                    lower = upper.T
                    out[blk, mid:, lo:mid] = lower
                    out[blk, lo:mid, mid:] = jnp.zeros_like(upper)
                    left = left_parts(lower, 1)
                    right = right_parts(upper)
                    rest = size - mid
                    for first in range(0, rest, 2 * TILE):
                        last = min(first + 2 * TILE, rest)
                        update = jnp.dot(
                            left[first:last], right[:, first:], preferred_element_type=jnp.float32
                        )
                        r = mid + first
                        work[blk, r : mid + last, r:] = work[blk, r : mid + last, r:] - update

        emit(k)
        return carry

    lax.fori_loop(0, tiles, step, 0)


def across(left, right):
    return lax.dot_general(
        left, right, (((1,), (1,)), ((), ())), preferred_element_type=jnp.float32
    )


def spread_body(points, targets, phase, freqs, phi, points_out, freqs_out, turns_out, projected,
                pbuf, tbuf, fbuf, fown, cbuf, flipped, turns, in_sem,
                psend, precv, tsend, trecv, fsend, frecv, csend, crecv, pass_sem,
                *, data_count, feat_count, scale):
    me = lax.axis_index("dp")
    here = lax.axis_index("feat")
    chips = data_count // 2
    chip, core = me // 2, me % 2
    rows = points.shape[0]
    depth, width = freqs.shape
    tile_width = freqs_out.shape[1]
    partner = chip * 2 + (1 - core)
    holder = me * tile_width // width
    offset = pl.multiple_of(me * tile_width % width, tile_width)
    pieces = cbuf.shape[0]
    piece = tile_width // pieces
    side_x = (here % 2 + holder % 2) % 2
    side_y = (here // 2 + holder // 2) % 2
    opposite = 3 - holder

    loads = [
        pltpu.make_async_copy(points, pbuf.at[me], in_sem.at[0]),
        pltpu.make_async_copy(targets, tbuf.at[me], in_sem.at[1]),
        pltpu.make_async_copy(phase, fbuf.at[here], in_sem.at[2]),
        pltpu.make_async_copy(freqs, fown, in_sem.at[3]),
    ]
    for copy in loads:
        copy.start()

    def remote(source, target, send, recv, dp, feat):
        return pltpu.make_async_remote_copy(
            src_ref=source, dst_ref=target, send_sem=send, recv_sem=recv,
            device_id={"dp": dp, "feat": feat}, device_id_type=pl.DeviceIdType.MESH)

    barrier = pltpu.get_barrier_semaphore()
    for step in range(1, data_count):
        pl.semaphore_signal(
            barrier, inc=1, device_id={"dp": lax.rem(me + step, data_count), "feat": here},
            device_id_type=pl.DeviceIdType.MESH)
    for step in range(1, feat_count):
        pl.semaphore_signal(
            barrier, inc=1, device_id={"dp": me, "feat": lax.rem(here + step, feat_count)},
            device_id_type=pl.DeviceIdType.MESH)
    pl.semaphore_wait(barrier, data_count + feat_count - 2)

    def peer(step):
        return lax.rem(chip + step, chips) * 2 + core

    def points_copy(slot, sem, dp):
        return remote(pbuf.at[slot], pbuf.at[slot], sem, precv.at[slot], dp, here)

    def targets_copy(slot, step):
        dp = lax.rem(me + step, data_count)
        return remote(tbuf.at[slot], tbuf.at[slot], tsend.at[step], trecv.at[slot], dp, here)

    def phase_copy(slot, step):
        feat = lax.rem(here + step, feat_count)
        return remote(fbuf.at[slot], fbuf.at[slot], fsend.at[step], frecv.at[slot], me, feat)

    def freqs_copy(q, way, feat):
        source = fown.at[:, pl.ds(offset + q * piece, piece)]
        return remote(source, cbuf.at[q], csend.at[way * pieces + q], crecv.at[q], me, feat)

    def freqs_pass(q, t):
        return remote(cbuf.at[q], cbuf.at[q], csend.at[t], crecv.at[q], me, opposite)

    order = [(t + 1) // 2 if t % 2 else chips - t // 2 for t in range(1, chips)]
    loads[0].wait()
    points_copy(me, psend.at[0], partner).start()
    for step in order:
        points_copy(me, psend.at[step], peer(step)).start()
    loads[1].wait()
    for step in range(1, data_count):
        targets_copy(me, step).start()
    loads[2].wait()
    for step in range(1, feat_count):
        phase_copy(here, step).start()
    loads[3].wait()
    near_x = (1 - holder % 2) + holder // 2 * 2
    near_y = holder % 2 + (1 - holder // 2) * 2
    sends = [(q, 0, near_x) for q in range(pieces)]
    sends += [((q + pieces // 2) % pieces, 1, near_y) for q in range(pieces)]
    half = pieces // 2

    @pl.when(here == holder)
    def _():
        for q, way, feat in sends:
            freqs_copy(q, way, feat).start()

    flipped[...] = fown[...].T
    for first in range(0, width, TILE):
        row = fbuf[here, :, first : first + TILE] * (0.5 / math.pi)
        turns[first : first + TILE, :] = jnp.broadcast_to(row, (TILE, TILE)).T
    projected[...] = jnp.zeros_like(projected)
    step_width = min(width, 1024)

    def compute(slot):
        at = pl.multiple_of(slot * rows, rows)
        block = pbuf[slot]
        points_out[pl.ds(at, rows), :] = block

        def part(j, carry):
            feats = pl.ds(pl.multiple_of(j * step_width, step_width), step_width)
            angle = across(flipped[feats, :], block) * (0.5 / math.pi)
            shift = turns[feats, :]
            value = wave(angle + jnp.concatenate([shift] * (rows // TILE), axis=1), scale)
            phi[feats, pl.ds(at, rows)] = value
            projected[:, feats] = projected[:, feats] + across(tbuf[slot], value)
            return carry

        lax.fori_loop(0, width // step_width, part, 0)

    def targets_wait(slot):
        remote(tbuf.at[slot], tbuf.at[slot], tsend.at[1], trecv.at[slot], partner, here).wait_recv()

    compute(me)
    points_copy(partner, psend.at[0], partner).wait_recv()
    targets_wait(partner)
    compute(partner)

    def arrive(t, carry):
        odd = t % 2
        step = odd * ((t + 1) // 2) + (1 - odd) * (chips - t // 2)
        source = lax.rem(chip + chips - step, chips)
        same = source * 2 + core
        other = source * 2 + (1 - core)
        points_copy(same, psend.at[0], partner).wait_recv()
        points_copy(same, pass_sem.at[t], partner).start()
        targets_wait(same)
        compute(same)
        points_copy(other, psend.at[0], partner).wait_recv()
        targets_wait(other)
        compute(other)

        @pl.when((side_x + side_y == 1) & (t <= half))
        def _():
            q = side_y * half + t - 1
            freqs_pass(q, 0).wait_recv()
            freqs_pass(q, t - 1).start()

        return carry

    lax.fori_loop(1, chips, arrive, 0)

    for step in range(1, feat_count):
        slot = lax.rem(here + step, feat_count)
        phase_copy(slot, step).wait_recv()
    turns_out[...] = fbuf[...] * (0.5 / math.pi)

    @pl.when(here == holder)
    def _():
        freqs_out[...] = fown[:, pl.ds(offset, tile_width)]
        for q, way, feat in sends:
            freqs_copy(q, way, feat).wait_send()

    @pl.when(side_x + side_y == 1)
    def _():
        for t in range(half):
            freqs_pass((1 - side_y) * half + t, 0).wait_recv()
            freqs_pass(side_y * half + t, t).wait_send()

    @pl.when(side_x + side_y == 2)
    def _():
        for q in range(pieces):
            freqs_pass(q, 0).wait_recv()

    @pl.when(here != holder)
    def _():
        for q in range(pieces):
            freqs_out[:, q * piece : (q + 1) * piece] = cbuf[q]

    points_copy(me, psend.at[0], partner).wait_send()
    for step in order:
        points_copy(me, psend.at[step], peer(step)).wait_send()
    for step in range(1, data_count):
        targets_copy(me, step).wait_send()
    for step in range(1, feat_count):
        phase_copy(here, step).wait_send()
    for t in range(1, chips):
        points_copy(me, pass_sem.at[t], partner).wait_send()


def spread(points, targets, phase, freqs, tile_width, scale):
    data_count, feat_count = lax.axis_size("dp"), lax.axis_size("feat")
    rows, depth = points.shape
    width = freqs.shape[1]
    outs = targets.shape[0]
    vmem = pl.BlockSpec(memory_space=pltpu.VMEM)
    hbm = pl.BlockSpec(memory_space=pltpu.HBM)
    dma = pltpu.SemaphoreType.DMA
    pieces = 4
    return pl.pallas_call(
        functools.partial(spread_body, data_count=data_count, feat_count=feat_count, scale=scale),
        out_shape=(
            jax.ShapeDtypeStruct((width, rows * data_count), jnp.bfloat16),
            jax.ShapeDtypeStruct((rows * data_count, depth), jnp.bfloat16),
            jax.ShapeDtypeStruct((depth, tile_width), jnp.bfloat16),
            jax.ShapeDtypeStruct((feat_count, 1, width), jnp.float32),
            jax.ShapeDtypeStruct((outs, width), jnp.float32),
        ),
        in_specs=[hbm] * 4,
        out_specs=[vmem] * 5,
        scratch_shapes=[
            pltpu.VMEM((data_count, rows, depth), jnp.bfloat16),
            pltpu.VMEM((data_count, outs, rows), jnp.bfloat16),
            pltpu.VMEM((feat_count, 1, width), jnp.float32),
            pltpu.VMEM((depth, width), jnp.bfloat16),
            pltpu.VMEM((pieces, depth, tile_width // pieces), jnp.bfloat16),
            pltpu.VMEM((width, depth), jnp.bfloat16),
            pltpu.VMEM((width, TILE), jnp.float32),
            dma((4,)),
            dma((data_count // 2,)),
            dma((data_count,)),
            dma((data_count,)),
            dma((data_count,)),
            dma((feat_count,)),
            dma((feat_count,)),
            dma((2 * pieces,)),
            dma((pieces,)),
            dma((data_count // 2,)),
        ],
        compiler_params=pltpu.CompilerParams(
            collective_id=0, has_side_effects=True, vmem_limit_bytes=24 * MIB
        ),
        cost_estimate=pl.CostEstimate(
            flops=2 * rows * data_count * depth * width,
            bytes_accessed=2 * rows * data_count * width,
            transcendentals=0,
        ),
        name="spread",
    )(points, targets, phase[None, :], freqs)


def assemble_body(phi, sums, ridge, points, freqs, phases, out, projected, gram,
                  work, block_out, packed, panel, cols_phi, ring, out_sem, ring_sem,
                  *, count, size, scale):
    projected[...] = sums[...]
    width, rows = phi.shape
    columns = freqs.shape[1]
    bands = TILE // BAND
    wide, down = columns // WIDE, width // WIDE
    parts = down // bands
    chunk = rows // down
    tall = bands * WIDE
    col_start = lax.axis_index("dp") * columns
    start = col_start - lax.axis_index("feat") * width
    holder = col_start // width
    offset = lax.rem(col_start, width)

    def make(j, r):
        cols = pl.ds(pl.multiple_of(j * WIDE, WIDE), WIDE)
        at = pl.ds(pl.multiple_of(r * chunk, chunk), chunk)
        cols_phi[lax.rem(j, 2), at, :] = features(
            points[at, :], freqs[:, cols],
            phases[holder, :, pl.ds(pl.multiple_of(offset + j * WIDE, WIDE), WIDE)], scale
        )

    def first(r, carry):
        make(0, r)
        return carry

    lax.fori_loop(0, down, first, 0)
    for blk in range(count):
        base = blk * size
        for c in range(0, size, WIDE):
            mid = c + WIDE
            tile = across(phi[base : base + mid, :], phi[base + c : base + mid, :])
            work[blk, :mid, c:mid] = with_ridge(tile, ridge[:, base + c : base + mid], 0, c)

    def rows_out(blk, k):
        at = pl.ds(pl.multiple_of(k * TILE, TILE), TILE)
        return pltpu.make_async_copy(block_out.at[blk, at], out.at[blk, at], out_sem.at[blk])

    def place(k):
        return k // parts, lax.rem(k, parts)

    def ring_out(k):
        j, part = place(k)
        slot = lax.rem(k, 2)
        return pltpu.make_async_copy(
            ring.at[slot],
            gram.at[pl.ds(pl.multiple_of(part * tall, tall), tall),
                    pl.ds(pl.multiple_of(j * WIDE, WIDE), WIDE)],
            ring_sem.at[slot])

    def begin(k):
        @pl.when(k >= 2)
        def _():
            ring_out(k).wait()

    def beside(k, band):
        j, part = place(k)
        r = part * bands + band
        at = pl.ds(pl.multiple_of(r * WIDE, WIDE), WIDE)
        ring[lax.rem(k, 2), band * WIDE : (band + 1) * WIDE, :] = jnp.dot(
            phi[at, :], cols_phi[lax.rem(j, 2)], preferred_element_type=jnp.float32
        )
        make(lax.rem(j + 1, wide), r)

    def emit(k):
        j, part = place(k)
        shift = start + j * WIDE - part * tall

        @pl.when((shift >= 0) & (shift < tall))
        def _():
            at = pl.ds(pl.multiple_of(shift, WIDE), WIDE)
            cols = pl.ds(pl.multiple_of(start + j * WIDE, WIDE), WIDE)
            slot = lax.rem(k, 2)
            ring[slot, at, :] = with_ridge(ring[slot, at, :], ridge[:, cols], 0, 0)

        ring_out(k).start()
        for blk in range(count):
            rows_out(blk, k).start()

    pair_steps(work, packed, panel, block_out, begin, beside, emit, size=size)
    tiles = size // TILE
    for k in range(tiles - 2, tiles):
        ring_out(k).wait()
    for blk in range(count):
        pltpu.make_async_copy(block_out.at[blk], out.at[blk], out_sem.at[blk]).wait()


def assemble(phi, sums, ridge, points, freqs, phases, size, scale):
    width, rows = phi.shape
    columns = freqs.shape[1]
    count = width // size
    outs = sums.shape[0]
    vmem = pl.BlockSpec(memory_space=pltpu.VMEM)
    hbm = pl.BlockSpec(memory_space=pltpu.HBM)
    return pl.pallas_call(
        functools.partial(assemble_body, count=count, size=size, scale=scale),
        out_shape=(
            jax.ShapeDtypeStruct((count, size, size), jnp.float32),
            jax.ShapeDtypeStruct((outs, width), jnp.float32),
            jax.ShapeDtypeStruct((width, columns), jnp.float32),
        ),
        in_specs=[vmem] * 6,
        out_specs=(hbm, vmem, hbm),
        scratch_shapes=[
            pltpu.VMEM((count, size, size), jnp.float32),
            pltpu.VMEM((count, size, size), jnp.float32),
            pltpu.VMEM((4, TILE, TILE), jnp.float32),
            pltpu.VMEM((count, TILE, TILE), jnp.float32),
            pltpu.VMEM((2, rows, WIDE), jnp.bfloat16),
            pltpu.VMEM((2, TILE // BAND * WIDE, WIDE), jnp.float32),
            pltpu.SemaphoreType.DMA((count,)),
            pltpu.SemaphoreType.DMA((2,)),
        ],
        compiler_params=pltpu.CompilerParams(vmem_limit_bytes=36 * MIB),
        cost_estimate=pl.CostEstimate(
            flops=30 * rows * width * size, bytes_accessed=8 * rows * width, transcendentals=0
        ),
        name="assemble",
    )(phi, sums, ridge, points, freqs, phases)


def near_shards(points, freqs, phase, ridge, targets):
    data_count, feat_count = lax.axis_size("dp"), lax.axis_size("feat")
    local_width = freqs.shape[1]
    tile_width = local_width * feat_count // data_count
    scale = math.sqrt(2.0 / (points.shape[0] * data_count))
    phi, points_all, col_freqs, turns, sums = spread(
        points, targets, phase, freqs, tile_width, scale
    )
    factors, projected, gram = assemble(
        phi, sums, ridge[None, :], points_all, col_freqs, turns, FB, scale
    )
    return gram, projected, factors.reshape(local_width, FB)


def lower_body(source, out, work, panel, sem, *, count, size):
    copy = pltpu.make_async_copy(source, work, sem)
    copy.start()
    copy.wait()
    factor_steps(work, panel, out, lambda k: None, count=count, size=size)


def lower_factors(blocks):
    count, size, _ = blocks.shape
    return pl.pallas_call(
        functools.partial(lower_body, count=count, size=size),
        out_shape=jax.ShapeDtypeStruct(blocks.shape, jnp.float32),
        in_specs=[pl.BlockSpec(memory_space=pl.ANY)],
        out_specs=pl.BlockSpec(memory_space=pltpu.VMEM),
        scratch_shapes=[
            pltpu.VMEM(blocks.shape, jnp.float32),
            pltpu.VMEM((count, TILE, 2 * TILE), jnp.float32),
            pltpu.SemaphoreType.DMA,
        ],
        compiler_params=pltpu.CompilerParams(vmem_limit_bytes=48 * MIB),
        name="lower_factors",
    )(blocks)


def wide_shards(points, freqs, phase, ridge, targets):
    data_count = lax.axis_size("dp")
    feat_count = lax.axis_size("feat")
    feat_index = lax.axis_index("feat")
    data_index = lax.axis_index("dp")
    local_width = freqs.shape[1]
    total_width = local_width * feat_count
    tile_width = total_width // data_count
    window = max(local_width, FB)
    window_start = feat_index * local_width // window * window
    row_start = feat_index * local_width
    col_start = data_index * tile_width
    scale = math.sqrt(2.0 / (points.shape[0] * data_count))
    points_all = lax.all_gather(points, "dp", axis=0, tiled=True)
    targets_all = lax.all_gather(targets, "dp", axis=1, tiled=True)
    freqs_all = lax.all_gather(freqs, "feat", axis=1, tiled=True)
    turns = phase * (0.5 / math.pi)
    turns_all, ridge_all = lax.all_gather(jnp.stack([turns, ridge]), "feat", axis=1, tiled=True)

    def features_at(start, width):
        return features(
            points_all,
            lax.dynamic_slice_in_dim(freqs_all, start, width, 1),
            lax.dynamic_slice_in_dim(turns_all, start, width, 0),
            scale,
        )

    window_phi = features_at(window_start, window)
    row_phi = lax.dynamic_slice_in_dim(window_phi, row_start - window_start, local_width, 1)
    window_ridge = lax.dynamic_slice_in_dim(ridge_all, window_start, window, 0)
    blocks = []
    for first in range(0, window, FB):
        part = window_phi[:, first : first + FB]
        block_ridge = window_ridge[first : first + FB, None]
        blocks.append(with_ridge(cross(part, part), block_ridge, 0, 0))
    factors_all = lower_factors(jnp.stack(blocks)).reshape(window, FB)
    factor_rows = lax.dynamic_slice_in_dim(factors_all, row_start - window_start, local_width, 0)
    col_phi = features_at(col_start, tile_width)
    gram_part = with_ridge(cross(row_phi, col_phi), ridge[:, None], row_start, col_start)
    projected = jnp.dot(targets_all, row_phi, preferred_element_type=jnp.float32)
    return gram_part, projected, factor_rows


def shards(points, freqs, phase, ridge, targets):
    local_width = freqs.shape[1]
    data_count, feat_count = lax.axis_size("dp"), lax.axis_size("feat")
    tile_width = local_width * feat_count // data_count
    near = (
        local_width == 2 * FB
        and local_width % tile_width == 0
        and tile_width % WIDE == 0
        and tile_width // WIDE * (local_width // WIDE) == FB // BAND
        and points.shape[0] * data_count % (local_width // WIDE) == 0
        and data_count % 2 == 0
        and feat_count == 4
    )
    return (near_shards if near else wide_shards)(points, freqs, phase, ridge, targets)


def solution(mesh):
    in_specs = (P("dp", None), P(None, "feat"), P("feat"), P("feat"), P(None, "dp"))
    out_specs = (P("feat", "dp"), P(None, "feat"), P("feat", None))
    return jax.shard_map(shards, mesh=mesh, in_specs=in_specs, out_specs=out_specs, check_vma=False)
```

```python
import functools
import math

import jax
import jax.numpy as jnp
from jax import lax
from jax.experimental import pallas as pl
from jax.experimental.pallas import tpu as pltpu
from jax.sharding import PartitionSpec as P

FB = 1024
TILE = 128
MICRO = 16
WIDE = 256
BAND = 32
SUBBAND = 16
SUBLANES = 8
HALF = TILE // 2
MIB = 1024 * 1024
COS_TURNS = (
    0.9999991998413438,
    -19.738978175861334,
    64.92858783993428,
    -85.27084362691367,
    58.786940763031694,
    -21.065429407523915,
)


def features(rows, freq_cols, phase_turns, scale):
    angle = jnp.dot(rows, freq_cols, preferred_element_type=jnp.float32)
    return wave(angle * (0.5 / math.pi) + phase_turns, scale)


def wave(turns, scale):
    part = turns - jnp.round(turns)
    square = part * part
    poly = square * (scale * COS_TURNS[-1]) + scale * COS_TURNS[-2]
    for coeff in COS_TURNS[-3::-1]:
        poly = poly * square + scale * coeff
    return poly.astype(jnp.bfloat16)


def cross(left, right):
    return lax.dot_general(
        left, right, (((0,), (0,)), ((), ())), preferred_element_type=jnp.float32
    )


def with_ridge(tile, ridge, row_start, col_start):
    rows_here = row_start + lax.broadcasted_iota(jnp.int32, tile.shape, 0)
    cols_here = col_start + lax.broadcasted_iota(jnp.int32, tile.shape, 1)
    return tile + jnp.where(rows_here == cols_here, ridge, 0.0)


def halves(value):
    high = value.astype(jnp.bfloat16)
    return high, (value - high.astype(jnp.float32)).astype(jnp.bfloat16)


def left_parts(value, axis):
    high, low = halves(value)
    return jnp.concatenate([high, high, low], axis=axis)


def right_parts(value):
    high, low = halves(value)
    return jnp.concatenate([high, low, high], axis=0)


def panel_rows(rows_lead, rows_tail, start):
    shape = rows_lead.shape
    row_ids = lax.broadcasted_iota(jnp.int32, shape, 0)
    cols = [
        jnp.broadcast_to(rows_lead[:, start + i : start + i + 1], shape) for i in range(MICRO)
    ]
    for i in range(MICRO):
        inv = lax.rsqrt(cols[i][i : i + 1, :])
        mult = cols[i] * inv
        for m in range(i + 1, MICRO):
            cols[m] = cols[m] - mult * mult[m : m + 1, :]
        below = jnp.where(row_ids > i, mult, 0.0)
        here = row_ids == i
        lead = rows_lead[i : i + 1, :] * inv
        tail = rows_tail[i : i + 1, :] * inv
        rows_lead = jnp.where(here, lead, rows_lead - below * lead)
        rows_tail = jnp.where(here, tail, rows_tail - below * tail)
    return rows_lead, rows_tail


def spread_row(value, row):
    return jnp.broadcast_to(value[row : row + 1, :], value.shape)


def pair_rows(groups, own, base):
    shape = (SUBLANES, TILE)
    row_ids = lax.broadcasted_iota(jnp.int32, shape, 0)
    lanes = lax.broadcasted_iota(jnp.int32, shape, 1)
    side = jnp.where(lanes < HALF, base, base + HALF)
    count = len(groups)
    size = count * SUBLANES
    for first in range(0, size, SUBBAND):
        span = range(first, first + SUBBAND)
        cols = {
            m: {
                g: jnp.take_along_axis(groups[g][own], side + m, axis=1)
                for g in range(m // SUBLANES, count)
            }
            for m in span
        }
        pivot = spread_row(cols[first][first // SUBLANES], first % SUBLANES)
        for i in span:
            gi, ri = divmod(i, SUBLANES)
            inv = lax.rsqrt(pivot)
            if i + 1 in span:
                gn, rn = divmod(i + 1, SUBLANES)
                step = spread_row(cols[i][gn], rn) * inv
                pivot = spread_row(cols[i + 1][gn], rn) - step * step
            mult = {g: cols[i][g] * inv for g in range(gi, count)}
            for m in range(i + 1, span.stop):
                gm, rm = divmod(m, SUBLANES)
                scalar = spread_row(mult[gm], rm)
                for g in range(gm, count):
                    cols[m][g] = cols[m][g] - mult[g] * scalar
            below = jnp.where(row_ids > ri, mult[gi], 0.0)
            here = row_ids == ri
            for x in range(len(groups[0])):
                lead = spread_row(groups[gi][x], ri) * inv
                groups[gi][x] = jnp.where(here, lead, groups[gi][x] - below * lead)
                for g in range(gi + 1, count):
                    groups[g][x] = groups[g][x] - mult[g] * lead
    return groups


def pair_panel(panel, beside):
    low = lax.broadcasted_iota(jnp.int32, (HALF, TILE), 1) < HALF
    for start in range(0, TILE, BAND):
        end = start + BAND
        beside(start // BAND)
        quarter = start // HALF
        parts = range(quarter, quarter + 3)
        groups = [
            [panel[x, r : r + SUBLANES, :] for x in parts]
            for r in range(start, end, SUBLANES)
        ]
        groups = pair_rows(groups, 0, start % HALF)
        for g, group in enumerate(groups):
            for x, value in zip(parts, group):
                panel[x, start + g * SUBLANES : start + (g + 1) * SUBLANES, :] = value
        bands = [jnp.concatenate([group[x] for group in groups], axis=0) for x in range(3)]
        right = right_parts(jnp.concatenate(bands, axis=1))
        for q in range(end // HALF, TILE // HALF):
            first = max(end - q * HALF, 0)
            update = cross(left_parts(bands[q - quarter], 0), right)
            for x in parts:
                at = (x - quarter) * TILE
                piece = jnp.where(
                    low[first:],
                    update[first:HALF, at : at + TILE],
                    update[HALF + first :, at : at + TILE],
                )
                rows = slice(q * HALF + first, (q + 1) * HALF)
                panel[x, rows, :] = panel[x, rows, :] - piece


def pair_steps(work, packed, panel, out, begin, beside, emit, *, size):
    tiles = size // TILE
    row_ids = lax.broadcasted_iota(jnp.int32, (TILE, TILE), 0)
    col_ids = lax.broadcasted_iota(jnp.int32, (TILE, TILE), 1)
    low = col_ids < HALF

    def swap(left, right):
        return (
            jnp.where(low, left, pltpu.roll(right, HALF, 1)),
            jnp.where(low, pltpu.roll(left, HALF, 1), right),
        )

    def step(k, carry):
        begin(k)
        at = pl.multiple_of(k * TILE, TILE)
        diagonal = [work[blk, pl.ds(at, TILE), pl.ds(at, TILE)] for blk in range(2)]
        packed[0], packed[1] = swap(*diagonal)
        packed[2] = jnp.where(row_ids == lax.rem(col_ids, HALF), 1.0, 0.0)
        packed[3] = jnp.where(row_ids == lax.rem(col_ids, HALF) + HALF, 1.0, 0.0)
        pair_panel(packed, functools.partial(beside, k))
        lead = swap(packed[0], packed[1])
        tail = swap(packed[2], packed[3])
        for blk in range(2):
            panel[blk] = tail[blk]
            lower = jnp.where(row_ids >= col_ids, lead[blk].T, 0.0)
            out[blk, pl.ds(at, TILE), pl.ds(at, TILE)] = lower
        for c in range(tiles - 1):

            @pl.when(k == c)
            def _():
                trailing(work, panel, out, c, 2, size)

        emit(k)
        return carry

    lax.fori_loop(0, tiles, step, 0)


def trailing(work, panel, out, c, count, size):
    lo, mid = c * TILE, (c + 1) * TILE
    for blk in range(count):
        upper = jnp.dot(
            left_parts(panel[blk], 1),
            right_parts(work[blk, lo:mid, mid:]),
            preferred_element_type=jnp.float32,
        )
        lower = upper.T
        out[blk, mid:, lo:mid] = lower
        out[blk, lo:mid, mid:] = jnp.zeros_like(upper)
        left = left_parts(lower, 1)
        right = right_parts(upper)
        rest = size - mid
        for first in range(0, rest, 2 * TILE):
            last = min(first + 2 * TILE, rest)
            update = jnp.dot(
                left[first:last], right[:, first:], preferred_element_type=jnp.float32
            )
            r = mid + first
            work[blk, r : mid + last, r:] = work[blk, r : mid + last, r:] - update


def factor_steps(work, panel, out, emit, *, count, size):
    tiles = size // TILE
    row_ids = lax.broadcasted_iota(jnp.int32, (TILE, TILE), 0)
    col_ids = lax.broadcasted_iota(jnp.int32, (TILE, TILE), 1)

    def step(k, carry):
        at = pl.multiple_of(k * TILE, TILE)
        for blk in range(count):
            panel[blk, :, :TILE] = work[blk, pl.ds(at, TILE), pl.ds(at, TILE)]
            panel[blk, :, TILE:] = jnp.where(row_ids == col_ids, 1.0, 0.0)
        for start in range(0, TILE, MICRO):
            end = start + MICRO
            for blk in range(count):
                lead, tail = panel_rows(
                    panel[blk, start:end, :TILE], panel[blk, start:end, TILE:], start
                )
                panel[blk, start:end, :TILE] = lead
                panel[blk, start:end, TILE:] = tail
                if end < TILE:
                    left = left_parts(lead, 0)
                    right = right_parts(jnp.concatenate([lead, tail], axis=1))
                    panel[blk, end:, :] = panel[blk, end:, :] - cross(left, right)[end:, :]
        for blk in range(count):
            lower = jnp.where(row_ids >= col_ids, panel[blk, :, :TILE].T, 0.0)
            out[blk, pl.ds(at, TILE), pl.ds(at, TILE)] = lower
        for c in range(tiles - 1):

            @pl.when(k == c)
            def _():
                lo, mid = c * TILE, (c + 1) * TILE
                for blk in range(count):
                    upper = jnp.dot(
                        left_parts(panel[blk, :, TILE:], 1),
                        right_parts(work[blk, lo:mid, mid:]),
                        preferred_element_type=jnp.float32,
                    )
                    lower = upper.T
                    out[blk, mid:, lo:mid] = lower
                    out[blk, lo:mid, mid:] = jnp.zeros_like(upper)
                    left = left_parts(lower, 1)
                    right = right_parts(upper)
                    rest = size - mid
                    for first in range(0, rest, 2 * TILE):
                        last = min(first + 2 * TILE, rest)
                        update = jnp.dot(
                            left[first:last], right[:, first:], preferred_element_type=jnp.float32
                        )
                        r = mid + first
                        work[blk, r : mid + last, r:] = work[blk, r : mid + last, r:] - update

        emit(k)
        return carry

    lax.fori_loop(0, tiles, step, 0)


def across(left, right):
    return lax.dot_general(
        left, right, (((1,), (1,)), ((), ())), preferred_element_type=jnp.float32
    )


def spread_body(points, targets, phase, freqs, phi, points_out, freqs_out, turns_out, projected,
                pbuf, tbuf, fbuf, fown, cbuf, flipped, turns, in_sem,
                psend, precv, tsend, trecv, fsend, frecv, csend, crecv, pass_sem,
                *, data_count, feat_count, scale):
    me = lax.axis_index("dp")
    here = lax.axis_index("feat")
    chips = data_count // 2
    chip, core = me // 2, me % 2
    rows = points.shape[0]
    depth, width = freqs.shape
    tile_width = freqs_out.shape[1]
    partner = chip * 2 + (1 - core)
    holder = me * tile_width // width
    offset = pl.multiple_of(me * tile_width % width, tile_width)
    pieces = cbuf.shape[0]
    piece = tile_width // pieces
    side_x = (here % 2 + holder % 2) % 2
    side_y = (here // 2 + holder // 2) % 2
    opposite = 3 - holder

    loads = [
        pltpu.make_async_copy(points, pbuf.at[me], in_sem.at[0]),
        pltpu.make_async_copy(targets, tbuf.at[me], in_sem.at[1]),
        pltpu.make_async_copy(phase, fbuf.at[here], in_sem.at[2]),
        pltpu.make_async_copy(freqs, fown, in_sem.at[3]),
    ]
    for copy in loads:
        copy.start()

    def remote(source, target, send, recv, dp, feat):
        return pltpu.make_async_remote_copy(
            src_ref=source, dst_ref=target, send_sem=send, recv_sem=recv,
            device_id={"dp": dp, "feat": feat}, device_id_type=pl.DeviceIdType.MESH)

    barrier = pltpu.get_barrier_semaphore()
    for step in range(1, data_count):
        pl.semaphore_signal(
            barrier, inc=1, device_id={"dp": lax.rem(me + step, data_count), "feat": here},
            device_id_type=pl.DeviceIdType.MESH)
    for step in range(1, feat_count):
        pl.semaphore_signal(
            barrier, inc=1, device_id={"dp": me, "feat": lax.rem(here + step, feat_count)},
            device_id_type=pl.DeviceIdType.MESH)
    pl.semaphore_wait(barrier, data_count + feat_count - 2)

    def peer(step):
        return lax.rem(chip + step, chips) * 2 + core

    def points_copy(slot, sem, dp):
        return remote(pbuf.at[slot], pbuf.at[slot], sem, precv.at[slot], dp, here)

    def targets_copy(slot, step):
        dp = lax.rem(me + step, data_count)
        return remote(tbuf.at[slot], tbuf.at[slot], tsend.at[step], trecv.at[slot], dp, here)

    def phase_copy(slot, step):
        feat = lax.rem(here + step, feat_count)
        return remote(fbuf.at[slot], fbuf.at[slot], fsend.at[step], frecv.at[slot], me, feat)

    def freqs_copy(q, way, feat):
        source = fown.at[:, pl.ds(offset + q * piece, piece)]
        return remote(source, cbuf.at[q], csend.at[way * pieces + q], crecv.at[q], me, feat)

    def freqs_pass(q, t):
        return remote(cbuf.at[q], cbuf.at[q], csend.at[t], crecv.at[q], me, opposite)

    order = [(t + 1) // 2 if t % 2 else chips - t // 2 for t in range(1, chips)]
    loads[0].wait()
    points_copy(me, psend.at[0], partner).start()
    for step in order:
        points_copy(me, psend.at[step], peer(step)).start()
    loads[1].wait()
    for step in range(1, data_count):
        targets_copy(me, step).start()
    loads[2].wait()
    for step in range(1, feat_count):
        phase_copy(here, step).start()
    loads[3].wait()
    near_x = (1 - holder % 2) + holder // 2 * 2
    near_y = holder % 2 + (1 - holder // 2) * 2
    sends = [(q, 0, near_x) for q in range(pieces)]
    sends += [((q + pieces // 2) % pieces, 1, near_y) for q in range(pieces)]
    half = pieces // 2

    @pl.when(here == holder)
    def _():
        for q, way, feat in sends:
            freqs_copy(q, way, feat).start()

    flipped[...] = fown[...].T
    for first in range(0, width, TILE):
        row = fbuf[here, :, first : first + TILE] * (0.5 / math.pi)
        turns[first : first + TILE, :] = jnp.broadcast_to(row, (TILE, TILE)).T
    projected[...] = jnp.zeros_like(projected)
    step_width = min(width, 1024)

    def compute(slot):
        at = pl.multiple_of(slot * rows, rows)
        block = pbuf[slot]
        points_out[pl.ds(at, rows), :] = block

        def part(j, carry):
            feats = pl.ds(pl.multiple_of(j * step_width, step_width), step_width)
            angle = across(flipped[feats, :], block) * (0.5 / math.pi)
            shift = turns[feats, :]
            value = wave(angle + jnp.concatenate([shift] * (rows // TILE), axis=1), scale)
            phi[feats, pl.ds(at, rows)] = value
            projected[:, feats] = projected[:, feats] + across(tbuf[slot], value)
            return carry

        lax.fori_loop(0, width // step_width, part, 0)

    def targets_wait(slot):
        remote(tbuf.at[slot], tbuf.at[slot], tsend.at[1], trecv.at[slot], partner, here).wait_recv()

    compute(me)
    points_copy(partner, psend.at[0], partner).wait_recv()
    targets_wait(partner)
    compute(partner)

    def arrive(t, carry):
        odd = t % 2
        step = odd * ((t + 1) // 2) + (1 - odd) * (chips - t // 2)
        source = lax.rem(chip + chips - step, chips)
        same = source * 2 + core
        other = source * 2 + (1 - core)
        points_copy(same, psend.at[0], partner).wait_recv()
        points_copy(same, pass_sem.at[t], partner).start()
        targets_wait(same)
        compute(same)
        points_copy(other, psend.at[0], partner).wait_recv()
        targets_wait(other)
        compute(other)

        @pl.when((side_x + side_y == 1) & (t <= half))
        def _():
            q = side_y * half + t - 1
            freqs_pass(q, 0).wait_recv()
            freqs_pass(q, t - 1).start()

        return carry

    lax.fori_loop(1, chips, arrive, 0)

    for step in range(1, feat_count):
        slot = lax.rem(here + step, feat_count)
        phase_copy(slot, step).wait_recv()
    turns_out[...] = fbuf[...] * (0.5 / math.pi)

    @pl.when(here == holder)
    def _():
        freqs_out[...] = fown[:, pl.ds(offset, tile_width)]
        for q, way, feat in sends:
            freqs_copy(q, way, feat).wait_send()

    @pl.when(side_x + side_y == 1)
    def _():
        for t in range(half):
            freqs_pass((1 - side_y) * half + t, 0).wait_recv()
            freqs_pass(side_y * half + t, t).wait_send()

    @pl.when(side_x + side_y == 2)
    def _():
        for q in range(pieces):
            freqs_pass(q, 0).wait_recv()

    @pl.when(here != holder)
    def _():
        for q in range(pieces):
            freqs_out[:, q * piece : (q + 1) * piece] = cbuf[q]

    points_copy(me, psend.at[0], partner).wait_send()
    for step in order:
        points_copy(me, psend.at[step], peer(step)).wait_send()
    for step in range(1, data_count):
        targets_copy(me, step).wait_send()
    for step in range(1, feat_count):
        phase_copy(here, step).wait_send()
    for t in range(1, chips):
        points_copy(me, pass_sem.at[t], partner).wait_send()


def spread(points, targets, phase, freqs, tile_width, scale):
    data_count, feat_count = lax.axis_size("dp"), lax.axis_size("feat")
    rows, depth = points.shape
    width = freqs.shape[1]
    outs = targets.shape[0]
    vmem = pl.BlockSpec(memory_space=pltpu.VMEM)
    hbm = pl.BlockSpec(memory_space=pltpu.HBM)
    dma = pltpu.SemaphoreType.DMA
    pieces = 4
    return pl.pallas_call(
        functools.partial(spread_body, data_count=data_count, feat_count=feat_count, scale=scale),
        out_shape=(
            jax.ShapeDtypeStruct((width, rows * data_count), jnp.bfloat16),
            jax.ShapeDtypeStruct((rows * data_count, depth), jnp.bfloat16),
            jax.ShapeDtypeStruct((depth, tile_width), jnp.bfloat16),
            jax.ShapeDtypeStruct((feat_count, 1, width), jnp.float32),
            jax.ShapeDtypeStruct((outs, width), jnp.float32),
        ),
        in_specs=[hbm] * 4,
        out_specs=[vmem] * 5,
        scratch_shapes=[
            pltpu.VMEM((data_count, rows, depth), jnp.bfloat16),
            pltpu.VMEM((data_count, outs, rows), jnp.bfloat16),
            pltpu.VMEM((feat_count, 1, width), jnp.float32),
            pltpu.VMEM((depth, width), jnp.bfloat16),
            pltpu.VMEM((pieces, depth, tile_width // pieces), jnp.bfloat16),
            pltpu.VMEM((width, depth), jnp.bfloat16),
            pltpu.VMEM((width, TILE), jnp.float32),
            dma((4,)),
            dma((data_count // 2,)),
            dma((data_count,)),
            dma((data_count,)),
            dma((data_count,)),
            dma((feat_count,)),
            dma((feat_count,)),
            dma((2 * pieces,)),
            dma((pieces,)),
            dma((data_count // 2,)),
        ],
        compiler_params=pltpu.CompilerParams(
            collective_id=0, has_side_effects=True, vmem_limit_bytes=24 * MIB
        ),
        cost_estimate=pl.CostEstimate(
            flops=2 * rows * data_count * depth * width,
            bytes_accessed=2 * rows * data_count * width,
            transcendentals=0,
        ),
        name="spread",
    )(points, targets, phase[None, :], freqs)


def assemble_body(phi, sums, ridge, points, freqs, phases, out, projected, gram,
                  work, block_out, packed, panel, cols_phi, ring, out_sem, ring_sem,
                  *, count, size, scale):
    projected[...] = sums[...]
    width, rows = phi.shape
    columns = freqs.shape[1]
    bands = TILE // BAND
    wide, down = columns // WIDE, width // WIDE
    parts = down // bands
    chunk = rows // down
    tall = bands * WIDE
    col_start = lax.axis_index("dp") * columns
    start = col_start - lax.axis_index("feat") * width
    holder = col_start // width
    offset = lax.rem(col_start, width)

    def make(j, r):
        cols = pl.ds(pl.multiple_of(j * WIDE, WIDE), WIDE)
        at = pl.ds(pl.multiple_of(r * chunk, chunk), chunk)
        cols_phi[lax.rem(j, 2), at, :] = features(
            points[at, :], freqs[:, cols],
            phases[holder, :, pl.ds(pl.multiple_of(offset + j * WIDE, WIDE), WIDE)], scale
        )

    for blk in range(count):
        base = blk * size
        for c in range(0, size, WIDE):
            make(0, (base + c) // WIDE)
            mid = c + WIDE
            tile = across(phi[base : base + mid, :], phi[base + c : base + mid, :])
            work[blk, :mid, c:mid] = with_ridge(tile, ridge[:, base + c : base + mid], 0, c)

    def rows_out(blk, k):
        at = pl.ds(pl.multiple_of(k * TILE, TILE), TILE)
        return pltpu.make_async_copy(block_out.at[blk, at], out.at[blk, at], out_sem.at[blk])

    def place(k):
        return k // parts, lax.rem(k, parts)

    def ring_out(k):
        j, part = place(k)
        slot = lax.rem(k, 2)
        return pltpu.make_async_copy(
            ring.at[slot],
            gram.at[pl.ds(pl.multiple_of(part * tall, tall), tall),
                    pl.ds(pl.multiple_of(j * WIDE, WIDE), WIDE)],
            ring_sem.at[slot])

    def begin(k):
        @pl.when(k >= 2)
        def _():
            ring_out(k).wait()

    def beside(k, band):
        j, part = place(k)
        r = part * bands + band
        at = pl.ds(pl.multiple_of(r * WIDE, WIDE), WIDE)
        ring[lax.rem(k, 2), band * WIDE : (band + 1) * WIDE, :] = jnp.dot(
            phi[at, :], cols_phi[lax.rem(j, 2)], preferred_element_type=jnp.float32
        )
        make(lax.rem(j + 1, wide), r)

    def emit(k):
        j, part = place(k)
        shift = start + j * WIDE - part * tall

        @pl.when((shift >= 0) & (shift < tall))
        def _():
            at = pl.ds(pl.multiple_of(shift, WIDE), WIDE)
            cols = pl.ds(pl.multiple_of(start + j * WIDE, WIDE), WIDE)
            slot = lax.rem(k, 2)
            ring[slot, at, :] = with_ridge(ring[slot, at, :], ridge[:, cols], 0, 0)

        ring_out(k).start()
        for blk in range(count):
            rows_out(blk, k).start()

    pair_steps(work, packed, panel, block_out, begin, beside, emit, size=size)
    tiles = size // TILE
    for k in range(tiles - 2, tiles):
        ring_out(k).wait()
    for blk in range(count):
        pltpu.make_async_copy(block_out.at[blk], out.at[blk], out_sem.at[blk]).wait()


def assemble(phi, sums, ridge, points, freqs, phases, size, scale):
    width, rows = phi.shape
    columns = freqs.shape[1]
    count = width // size
    outs = sums.shape[0]
    vmem = pl.BlockSpec(memory_space=pltpu.VMEM)
    hbm = pl.BlockSpec(memory_space=pltpu.HBM)
    return pl.pallas_call(
        functools.partial(assemble_body, count=count, size=size, scale=scale),
        out_shape=(
            jax.ShapeDtypeStruct((count, size, size), jnp.float32),
            jax.ShapeDtypeStruct((outs, width), jnp.float32),
            jax.ShapeDtypeStruct((width, columns), jnp.float32),
        ),
        in_specs=[vmem] * 6,
        out_specs=(hbm, vmem, hbm),
        scratch_shapes=[
            pltpu.VMEM((count, size, size), jnp.float32),
            pltpu.VMEM((count, size, size), jnp.float32),
            pltpu.VMEM((4, TILE, TILE), jnp.float32),
            pltpu.VMEM((count, TILE, TILE), jnp.float32),
            pltpu.VMEM((2, rows, WIDE), jnp.bfloat16),
            pltpu.VMEM((2, TILE // BAND * WIDE, WIDE), jnp.float32),
            pltpu.SemaphoreType.DMA((count,)),
            pltpu.SemaphoreType.DMA((2,)),
        ],
        compiler_params=pltpu.CompilerParams(vmem_limit_bytes=36 * MIB),
        cost_estimate=pl.CostEstimate(
            flops=30 * rows * width * size, bytes_accessed=8 * rows * width, transcendentals=0
        ),
        name="assemble",
    )(phi, sums, ridge, points, freqs, phases)


def near_shards(points, freqs, phase, ridge, targets):
    data_count, feat_count = lax.axis_size("dp"), lax.axis_size("feat")
    local_width = freqs.shape[1]
    tile_width = local_width * feat_count // data_count
    scale = math.sqrt(2.0 / (points.shape[0] * data_count))
    phi, points_all, col_freqs, turns, sums = spread(
        points, targets, phase, freqs, tile_width, scale
    )
    factors, projected, gram = assemble(
        phi, sums, ridge[None, :], points_all, col_freqs, turns, FB, scale
    )
    return gram, projected, factors.reshape(local_width, FB)


def lower_body(source, out, work, panel, sem, *, count, size):
    copy = pltpu.make_async_copy(source, work, sem)
    copy.start()
    copy.wait()
    factor_steps(work, panel, out, lambda k: None, count=count, size=size)


def lower_factors(blocks):
    count, size, _ = blocks.shape
    return pl.pallas_call(
        functools.partial(lower_body, count=count, size=size),
        out_shape=jax.ShapeDtypeStruct(blocks.shape, jnp.float32),
        in_specs=[pl.BlockSpec(memory_space=pl.ANY)],
        out_specs=pl.BlockSpec(memory_space=pltpu.VMEM),
        scratch_shapes=[
            pltpu.VMEM(blocks.shape, jnp.float32),
            pltpu.VMEM((count, TILE, 2 * TILE), jnp.float32),
            pltpu.SemaphoreType.DMA,
        ],
        compiler_params=pltpu.CompilerParams(vmem_limit_bytes=48 * MIB),
        name="lower_factors",
    )(blocks)


def wide_shards(points, freqs, phase, ridge, targets):
    data_count = lax.axis_size("dp")
    feat_count = lax.axis_size("feat")
    feat_index = lax.axis_index("feat")
    data_index = lax.axis_index("dp")
    local_width = freqs.shape[1]
    total_width = local_width * feat_count
    tile_width = total_width // data_count
    window = max(local_width, FB)
    window_start = feat_index * local_width // window * window
    row_start = feat_index * local_width
    col_start = data_index * tile_width
    scale = math.sqrt(2.0 / (points.shape[0] * data_count))
    points_all = lax.all_gather(points, "dp", axis=0, tiled=True)
    targets_all = lax.all_gather(targets, "dp", axis=1, tiled=True)
    freqs_all = lax.all_gather(freqs, "feat", axis=1, tiled=True)
    turns = phase * (0.5 / math.pi)
    turns_all, ridge_all = lax.all_gather(jnp.stack([turns, ridge]), "feat", axis=1, tiled=True)

    def features_at(start, width):
        return features(
            points_all,
            lax.dynamic_slice_in_dim(freqs_all, start, width, 1),
            lax.dynamic_slice_in_dim(turns_all, start, width, 0),
            scale,
        )

    window_phi = features_at(window_start, window)
    row_phi = lax.dynamic_slice_in_dim(window_phi, row_start - window_start, local_width, 1)
    window_ridge = lax.dynamic_slice_in_dim(ridge_all, window_start, window, 0)
    blocks = []
    for first in range(0, window, FB):
        part = window_phi[:, first : first + FB]
        block_ridge = window_ridge[first : first + FB, None]
        blocks.append(with_ridge(cross(part, part), block_ridge, 0, 0))
    factors_all = lower_factors(jnp.stack(blocks)).reshape(window, FB)
    factor_rows = lax.dynamic_slice_in_dim(factors_all, row_start - window_start, local_width, 0)
    col_phi = features_at(col_start, tile_width)
    gram_part = with_ridge(cross(row_phi, col_phi), ridge[:, None], row_start, col_start)
    projected = jnp.dot(targets_all, row_phi, preferred_element_type=jnp.float32)
    return gram_part, projected, factor_rows


def shards(points, freqs, phase, ridge, targets):
    local_width = freqs.shape[1]
    data_count, feat_count = lax.axis_size("dp"), lax.axis_size("feat")
    tile_width = local_width * feat_count // data_count
    near = (
        local_width == 2 * FB
        and local_width % tile_width == 0
        and tile_width % WIDE == 0
        and tile_width // WIDE * (local_width // WIDE) == FB // BAND
        and points.shape[0] * data_count % (local_width // WIDE) == 0
        and data_count % 2 == 0
        and feat_count == 4
    )
    return (near_shards if near else wide_shards)(points, freqs, phase, ridge, targets)


def solution(mesh):
    in_specs = (P("dp", None), P(None, "feat"), P("feat"), P("feat"), P(None, "dp"))
    out_specs = (P("feat", "dp"), P(None, "feat"), P("feat", None))
    return jax.shard_map(shards, mesh=mesh, in_specs=in_specs, out_specs=out_specs, check_vma=False)
```

```python
import functools
import math

import jax
import jax.numpy as jnp
from jax import lax
from jax.experimental import pallas as pl
from jax.experimental.pallas import tpu as pltpu
from jax.sharding import PartitionSpec as P

FB = 1024
TILE = 128
MICRO = 16
WIDE = 256
BAND = 32
SUBBAND = 16
SUBLANES = 8
HALF = TILE // 2
MIB = 1024 * 1024
COS_TURNS = (
    0.9999991998413438,
    -19.738978175861334,
    64.92858783993428,
    -85.27084362691367,
    58.786940763031694,
    -21.065429407523915,
)


def features(rows, freq_cols, phase_turns, scale):
    angle = jnp.dot(rows, freq_cols, preferred_element_type=jnp.float32)
    return wave(angle * (0.5 / math.pi) + phase_turns, scale)


def wave(turns, scale):
    part = turns - jnp.round(turns)
    square = part * part
    poly = square * (scale * COS_TURNS[-1]) + scale * COS_TURNS[-2]
    for coeff in COS_TURNS[-3::-1]:
        poly = poly * square + scale * coeff
    return poly.astype(jnp.bfloat16)


def cross(left, right):
    return lax.dot_general(
        left, right, (((0,), (0,)), ((), ())), preferred_element_type=jnp.float32
    )


def with_ridge(tile, ridge, row_start, col_start):
    rows_here = row_start + lax.broadcasted_iota(jnp.int32, tile.shape, 0)
    cols_here = col_start + lax.broadcasted_iota(jnp.int32, tile.shape, 1)
    return tile + jnp.where(rows_here == cols_here, ridge, 0.0)


def halves(value):
    high = value.astype(jnp.bfloat16)
    return high, (value - high.astype(jnp.float32)).astype(jnp.bfloat16)


def left_parts(value, axis):
    high, low = halves(value)
    return jnp.concatenate([high, high, low], axis=axis)


def right_parts(value):
    high, low = halves(value)
    return jnp.concatenate([high, low, high], axis=0)


def panel_rows(rows_lead, rows_tail, start):
    shape = rows_lead.shape
    row_ids = lax.broadcasted_iota(jnp.int32, shape, 0)
    cols = [
        jnp.broadcast_to(rows_lead[:, start + i : start + i + 1], shape) for i in range(MICRO)
    ]
    for i in range(MICRO):
        inv = lax.rsqrt(cols[i][i : i + 1, :])
        mult = cols[i] * inv
        for m in range(i + 1, MICRO):
            cols[m] = cols[m] - mult * mult[m : m + 1, :]
        below = jnp.where(row_ids > i, mult, 0.0)
        here = row_ids == i
        lead = rows_lead[i : i + 1, :] * inv
        tail = rows_tail[i : i + 1, :] * inv
        rows_lead = jnp.where(here, lead, rows_lead - below * lead)
        rows_tail = jnp.where(here, tail, rows_tail - below * tail)
    return rows_lead, rows_tail


def spread_row(value, row):
    return jnp.broadcast_to(value[row : row + 1, :], value.shape)


def pair_rows(groups, own, base):
    shape = (SUBLANES, TILE)
    row_ids = lax.broadcasted_iota(jnp.int32, shape, 0)
    lanes = lax.broadcasted_iota(jnp.int32, shape, 1)
    side = jnp.where(lanes < HALF, base, base + HALF)
    count = len(groups)
    size = count * SUBLANES
    for first in range(0, size, SUBBAND):
        span = range(first, first + SUBBAND)
        cols = {
            m: {
                g: jnp.take_along_axis(groups[g][own], side + m, axis=1)
                for g in range(m // SUBLANES, count)
            }
            for m in span
        }
        pivot = spread_row(cols[first][first // SUBLANES], first % SUBLANES)
        for i in span:
            gi, ri = divmod(i, SUBLANES)
            inv = lax.rsqrt(pivot)
            if i + 1 in span:
                gn, rn = divmod(i + 1, SUBLANES)
                step = spread_row(cols[i][gn], rn) * inv
                pivot = spread_row(cols[i + 1][gn], rn) - step * step
            mult = {g: cols[i][g] * inv for g in range(gi, count)}
            for m in range(i + 1, span.stop):
                gm, rm = divmod(m, SUBLANES)
                scalar = spread_row(mult[gm], rm)
                for g in range(gm, count):
                    cols[m][g] = cols[m][g] - mult[g] * scalar
            below = jnp.where(row_ids > ri, mult[gi], 0.0)
            here = row_ids == ri
            for x in range(len(groups[0])):
                lead = spread_row(groups[gi][x], ri) * inv
                groups[gi][x] = jnp.where(here, lead, groups[gi][x] - below * lead)
                for g in range(gi + 1, count):
                    groups[g][x] = groups[g][x] - mult[g] * lead
    return groups


def pair_panel(panel, beside):
    low = lax.broadcasted_iota(jnp.int32, (HALF, TILE), 1) < HALF
    for start in range(0, TILE, BAND):
        end = start + BAND
        beside(start // BAND)
        quarter = start // HALF
        parts = range(quarter, quarter + 3)
        groups = [
            [panel[x, r : r + SUBLANES, :] for x in parts]
            for r in range(start, end, SUBLANES)
        ]
        groups = pair_rows(groups, 0, start % HALF)
        for g, group in enumerate(groups):
            for x, value in zip(parts, group):
                panel[x, start + g * SUBLANES : start + (g + 1) * SUBLANES, :] = value
        bands = [jnp.concatenate([group[x] for group in groups], axis=0) for x in range(3)]
        right = right_parts(jnp.concatenate(bands, axis=1))
        for q in range(end // HALF, TILE // HALF):
            first = max(end - q * HALF, 0)
            update = cross(left_parts(bands[q - quarter], 0), right)
            for x in parts:
                at = (x - quarter) * TILE
                piece = jnp.where(
                    low[first:],
                    update[first:HALF, at : at + TILE],
                    update[HALF + first :, at : at + TILE],
                )
                rows = slice(q * HALF + first, (q + 1) * HALF)
                panel[x, rows, :] = panel[x, rows, :] - piece


def pair_steps(work, packed, panel, out, begin, beside, emit, *, size):
    tiles = size // TILE
    row_ids = lax.broadcasted_iota(jnp.int32, (TILE, TILE), 0)
    col_ids = lax.broadcasted_iota(jnp.int32, (TILE, TILE), 1)
    low = col_ids < HALF

    def swap(left, right):
        return (
            jnp.where(low, left, pltpu.roll(right, HALF, 1)),
            jnp.where(low, pltpu.roll(left, HALF, 1), right),
        )

    def step(k, carry):
        begin(k)
        at = pl.multiple_of(k * TILE, TILE)
        diagonal = [work[blk, pl.ds(at, TILE), pl.ds(at, TILE)] for blk in range(2)]
        packed[0], packed[1] = swap(*diagonal)
        packed[2] = jnp.where(row_ids == lax.rem(col_ids, HALF), 1.0, 0.0)
        packed[3] = jnp.where(row_ids == lax.rem(col_ids, HALF) + HALF, 1.0, 0.0)
        pair_panel(packed, functools.partial(beside, k))
        lead = swap(packed[0], packed[1])
        tail = swap(packed[2], packed[3])
        for blk in range(2):
            panel[blk] = tail[blk]
            lower = jnp.where(row_ids >= col_ids, lead[blk].T, 0.0)
            out[blk, pl.ds(at, TILE), pl.ds(at, TILE)] = lower
        for c in range(tiles - 1):

            @pl.when(k == c)
            def _():
                trailing(work, panel, out, c, 2, size)

        emit(k)
        return carry

    lax.fori_loop(0, tiles, step, 0)


def trailing(work, panel, out, c, count, size):
    lo, mid = c * TILE, (c + 1) * TILE
    for blk in range(count):
        upper = jnp.dot(
            left_parts(panel[blk], 1),
            right_parts(work[blk, lo:mid, mid:]),
            preferred_element_type=jnp.float32,
        )
        lower = upper.T
        out[blk, mid:, lo:mid] = lower
        out[blk, lo:mid, mid:] = jnp.zeros_like(upper)
        left = left_parts(lower, 1)
        right = right_parts(upper)
        rest = size - mid
        for first in range(0, rest, 2 * TILE):
            last = min(first + 2 * TILE, rest)
            update = jnp.dot(
                left[first:last], right[:, first:], preferred_element_type=jnp.float32
            )
            r = mid + first
            work[blk, r : mid + last, r:] = work[blk, r : mid + last, r:] - update


def factor_steps(work, panel, out, emit, *, count, size):
    tiles = size // TILE
    row_ids = lax.broadcasted_iota(jnp.int32, (TILE, TILE), 0)
    col_ids = lax.broadcasted_iota(jnp.int32, (TILE, TILE), 1)

    def step(k, carry):
        at = pl.multiple_of(k * TILE, TILE)
        for blk in range(count):
            panel[blk, :, :TILE] = work[blk, pl.ds(at, TILE), pl.ds(at, TILE)]
            panel[blk, :, TILE:] = jnp.where(row_ids == col_ids, 1.0, 0.0)
        for start in range(0, TILE, MICRO):
            end = start + MICRO
            for blk in range(count):
                lead, tail = panel_rows(
                    panel[blk, start:end, :TILE], panel[blk, start:end, TILE:], start
                )
                panel[blk, start:end, :TILE] = lead
                panel[blk, start:end, TILE:] = tail
                if end < TILE:
                    left = left_parts(lead, 0)
                    right = right_parts(jnp.concatenate([lead, tail], axis=1))
                    panel[blk, end:, :] = panel[blk, end:, :] - cross(left, right)[end:, :]
        for blk in range(count):
            lower = jnp.where(row_ids >= col_ids, panel[blk, :, :TILE].T, 0.0)
            out[blk, pl.ds(at, TILE), pl.ds(at, TILE)] = lower
        for c in range(tiles - 1):

            @pl.when(k == c)
            def _():
                lo, mid = c * TILE, (c + 1) * TILE
                for blk in range(count):
                    upper = jnp.dot(
                        left_parts(panel[blk, :, TILE:], 1),
                        right_parts(work[blk, lo:mid, mid:]),
                        preferred_element_type=jnp.float32,
                    )
                    lower = upper.T
                    out[blk, mid:, lo:mid] = lower
                    out[blk, lo:mid, mid:] = jnp.zeros_like(upper)
                    left = left_parts(lower, 1)
                    right = right_parts(upper)
                    rest = size - mid
                    for first in range(0, rest, 2 * TILE):
                        last = min(first + 2 * TILE, rest)
                        update = jnp.dot(
                            left[first:last], right[:, first:], preferred_element_type=jnp.float32
                        )
                        r = mid + first
                        work[blk, r : mid + last, r:] = work[blk, r : mid + last, r:] - update

        emit(k)
        return carry

    lax.fori_loop(0, tiles, step, 0)


def across(left, right):
    return lax.dot_general(
        left, right, (((1,), (1,)), ((), ())), preferred_element_type=jnp.float32
    )


def spread_body(points, targets, phase, freqs, phi, points_out, freqs_out, turns_out, projected,
                pbuf, tbuf, fbuf, cbuf, flipped, turns, in_sem,
                psend, precv, tsend, trecv, fsend, frecv, csend, crecv, pass_sem,
                *, data_count, feat_count, scale):
    me = lax.axis_index("dp")
    here = lax.axis_index("feat")
    chips = data_count // 2
    chip, core = me // 2, me % 2
    rows = points.shape[0]
    depth, width = freqs.shape
    tile_width = freqs_out.shape[1]
    partner = chip * 2 + (1 - core)
    holder = me * tile_width // width
    offset = pl.multiple_of(me * tile_width % width, tile_width)
    pieces = cbuf.shape[0]
    piece = tile_width // pieces
    side_x = (here % 2 + holder % 2) % 2
    side_y = (here // 2 + holder // 2) % 2
    opposite = 3 - holder

    loads = [
        pltpu.make_async_copy(points, pbuf.at[me], in_sem.at[0]),
        pltpu.make_async_copy(targets, tbuf.at[me], in_sem.at[1]),
        pltpu.make_async_copy(phase, fbuf.at[here], in_sem.at[2]),
    ]
    for copy in loads:
        copy.start()

    def remote(source, target, send, recv, dp, feat):
        return pltpu.make_async_remote_copy(
            src_ref=source, dst_ref=target, send_sem=send, recv_sem=recv,
            device_id={"dp": dp, "feat": feat}, device_id_type=pl.DeviceIdType.MESH)

    barrier = pltpu.get_barrier_semaphore()
    for step in range(1, data_count):
        pl.semaphore_signal(
            barrier, inc=1, device_id={"dp": lax.rem(me + step, data_count), "feat": here},
            device_id_type=pl.DeviceIdType.MESH)
    for step in range(1, feat_count):
        pl.semaphore_signal(
            barrier, inc=1, device_id={"dp": me, "feat": lax.rem(here + step, feat_count)},
            device_id_type=pl.DeviceIdType.MESH)
    pl.semaphore_wait(barrier, data_count + feat_count - 2)

    def peer(step):
        return lax.rem(chip + step, chips) * 2 + core

    def points_copy(slot, sem, dp):
        return remote(pbuf.at[slot], pbuf.at[slot], sem, precv.at[slot], dp, here)

    def targets_copy(slot, step):
        dp = lax.rem(me + step, data_count)
        return remote(tbuf.at[slot], tbuf.at[slot], tsend.at[step], trecv.at[slot], dp, here)

    def phase_copy(slot, step):
        feat = lax.rem(here + step, feat_count)
        return remote(fbuf.at[slot], fbuf.at[slot], fsend.at[step], frecv.at[slot], me, feat)

    def freqs_copy(q, way, feat):
        source = freqs.at[:, pl.ds(offset + q * piece, piece)]
        return remote(source, cbuf.at[q], csend.at[way * pieces + q], crecv.at[q], me, feat)

    def freqs_pass(q, t):
        return remote(cbuf.at[q], cbuf.at[q], csend.at[t], crecv.at[q], me, opposite)

    order = [(t + 1) // 2 if t % 2 else chips - t // 2 for t in range(1, chips)]
    loads[0].wait()
    points_copy(me, psend.at[0], partner).start()
    for step in order:
        points_copy(me, psend.at[step], peer(step)).start()
    loads[1].wait()
    for step in range(1, data_count):
        targets_copy(me, step).start()
    loads[2].wait()
    for step in range(1, feat_count):
        phase_copy(here, step).start()
    near_x = (1 - holder % 2) + holder // 2 * 2
    near_y = holder % 2 + (1 - holder // 2) * 2
    sends = [(q, 0, near_x) for q in range(pieces)]
    sends += [((q + pieces // 2) % pieces, 1, near_y) for q in range(pieces)]
    half = pieces // 2

    @pl.when(here == holder)
    def _():
        for q, way, feat in sends:
            freqs_copy(q, way, feat).start()

    flipped[...] = freqs[...].T
    for first in range(0, width, TILE):
        row = fbuf[here, :, first : first + TILE] * (0.5 / math.pi)
        turns[first : first + TILE, :] = jnp.broadcast_to(row, (TILE, TILE)).T
    projected[...] = jnp.zeros_like(projected)
    step_width = min(width, 1024)

    def compute(slot):
        at = pl.multiple_of(slot * rows, rows)
        block = pbuf[slot]
        points_out[pl.ds(at, rows), :] = block

        def part(j, carry):
            feats = pl.ds(pl.multiple_of(j * step_width, step_width), step_width)
            angle = across(flipped[feats, :], block) * (0.5 / math.pi)
            shift = turns[feats, :]
            value = wave(angle + jnp.concatenate([shift] * (rows // TILE), axis=1), scale)
            phi[feats, pl.ds(at, rows)] = value
            projected[:, feats] = projected[:, feats] + across(tbuf[slot], value)
            return carry

        lax.fori_loop(0, width // step_width, part, 0)

    def targets_wait(slot):
        remote(tbuf.at[slot], tbuf.at[slot], tsend.at[1], trecv.at[slot], partner, here).wait_recv()

    compute(me)
    points_copy(partner, psend.at[0], partner).wait_recv()
    targets_wait(partner)
    compute(partner)

    def arrive(t, carry):
        odd = t % 2
        step = odd * ((t + 1) // 2) + (1 - odd) * (chips - t // 2)
        source = lax.rem(chip + chips - step, chips)
        same = source * 2 + core
        other = source * 2 + (1 - core)
        points_copy(same, psend.at[0], partner).wait_recv()
        points_copy(same, pass_sem.at[t], partner).start()
        targets_wait(same)
        compute(same)
        points_copy(other, psend.at[0], partner).wait_recv()
        targets_wait(other)
        compute(other)

        @pl.when((side_x + side_y == 1) & (t <= half))
        def _():
            q = side_y * half + t - 1
            freqs_pass(q, 0).wait_recv()
            freqs_pass(q, t - 1).start()

        return carry

    lax.fori_loop(1, chips, arrive, 0)

    for step in range(1, feat_count):
        slot = lax.rem(here + step, feat_count)
        phase_copy(slot, step).wait_recv()
    turns_out[...] = fbuf[...] * (0.5 / math.pi)

    @pl.when(here == holder)
    def _():
        freqs_out[...] = freqs[:, pl.ds(offset, tile_width)]
        for q, way, feat in sends:
            freqs_copy(q, way, feat).wait_send()

    @pl.when(side_x + side_y == 1)
    def _():
        for t in range(half):
            freqs_pass((1 - side_y) * half + t, 0).wait_recv()
            freqs_pass(side_y * half + t, t).wait_send()

    @pl.when(side_x + side_y == 2)
    def _():
        for q in range(pieces):
            freqs_pass(q, 0).wait_recv()

    @pl.when(here != holder)
    def _():
        for q in range(pieces):
            freqs_out[:, q * piece : (q + 1) * piece] = cbuf[q]

    points_copy(me, psend.at[0], partner).wait_send()
    for step in order:
        points_copy(me, psend.at[step], peer(step)).wait_send()
    for step in range(1, data_count):
        targets_copy(me, step).wait_send()
    for step in range(1, feat_count):
        phase_copy(here, step).wait_send()
    for t in range(1, chips):
        points_copy(me, pass_sem.at[t], partner).wait_send()


def spread(points, targets, phase, freqs, tile_width, scale):
    data_count, feat_count = lax.axis_size("dp"), lax.axis_size("feat")
    rows, depth = points.shape
    width = freqs.shape[1]
    outs = targets.shape[0]
    vmem = pl.BlockSpec(memory_space=pltpu.VMEM)
    hbm = pl.BlockSpec(memory_space=pltpu.HBM)
    dma = pltpu.SemaphoreType.DMA
    pieces = 4
    return pl.pallas_call(
        functools.partial(spread_body, data_count=data_count, feat_count=feat_count, scale=scale),
        out_shape=(
            jax.ShapeDtypeStruct((width, rows * data_count), jnp.bfloat16),
            jax.ShapeDtypeStruct((rows * data_count, depth), jnp.bfloat16),
            jax.ShapeDtypeStruct((depth, tile_width), jnp.bfloat16),
            jax.ShapeDtypeStruct((feat_count, 1, width), jnp.float32),
            jax.ShapeDtypeStruct((outs, width), jnp.float32),
        ),
        in_specs=[hbm] * 3 + [vmem],
        out_specs=[vmem] * 5,
        scratch_shapes=[
            pltpu.VMEM((data_count, rows, depth), jnp.bfloat16),
            pltpu.VMEM((data_count, outs, rows), jnp.bfloat16),
            pltpu.VMEM((feat_count, 1, width), jnp.float32),
            pltpu.VMEM((pieces, depth, tile_width // pieces), jnp.bfloat16),
            pltpu.VMEM((width, depth), jnp.bfloat16),
            pltpu.VMEM((width, TILE), jnp.float32),
            dma((3,)),
            dma((data_count // 2,)),
            dma((data_count,)),
            dma((data_count,)),
            dma((data_count,)),
            dma((feat_count,)),
            dma((feat_count,)),
            dma((2 * pieces,)),
            dma((pieces,)),
            dma((data_count // 2,)),
        ],
        compiler_params=pltpu.CompilerParams(
            collective_id=0, has_side_effects=True, vmem_limit_bytes=24 * MIB
        ),
        cost_estimate=pl.CostEstimate(
            flops=2 * rows * data_count * depth * width,
            bytes_accessed=2 * rows * data_count * width,
            transcendentals=0,
        ),
        name="spread",
    )(points, targets, phase[None, :], freqs)


def assemble_body(phi, sums, ridge, points, freqs, phases, out, projected, gram,
                  work, block_out, packed, panel, cols_phi, ring, out_sem, ring_sem,
                  *, count, size, scale):
    projected[...] = sums[...]
    width, rows = phi.shape
    columns = freqs.shape[1]
    bands = TILE // BAND
    wide, down = columns // WIDE, width // WIDE
    parts = down // bands
    chunk = rows // down
    tall = bands * WIDE
    col_start = lax.axis_index("dp") * columns
    start = col_start - lax.axis_index("feat") * width
    holder = col_start // width
    offset = lax.rem(col_start, width)

    def make(j, r):
        cols = pl.ds(pl.multiple_of(j * WIDE, WIDE), WIDE)
        at = pl.ds(pl.multiple_of(r * chunk, chunk), chunk)
        cols_phi[lax.rem(j, 2), at, :] = features(
            points[at, :], freqs[:, cols],
            phases[holder, :, pl.ds(pl.multiple_of(offset + j * WIDE, WIDE), WIDE)], scale
        )

    for blk in range(count):
        base = blk * size
        for c in range(0, size, WIDE):
            make(0, (base + c) // WIDE)
            mid = c + WIDE
            tile = across(phi[base : base + mid, :], phi[base + c : base + mid, :])
            work[blk, :mid, c:mid] = with_ridge(tile, ridge[:, base + c : base + mid], 0, c)

    def rows_out(blk, k):
        at = pl.ds(pl.multiple_of(k * TILE, TILE), TILE)
        return pltpu.make_async_copy(block_out.at[blk, at], out.at[blk, at], out_sem.at[blk])

    def place(k):
        return k // parts, lax.rem(k, parts)

    def ring_out(k):
        j, part = place(k)
        slot = lax.rem(k, 2)
        return pltpu.make_async_copy(
            ring.at[slot],
            gram.at[pl.ds(pl.multiple_of(part * tall, tall), tall),
                    pl.ds(pl.multiple_of(j * WIDE, WIDE), WIDE)],
            ring_sem.at[slot])

    def begin(k):
        @pl.when(k >= 2)
        def _():
            ring_out(k).wait()

    def beside(k, band):
        j, part = place(k)
        r = part * bands + band
        at = pl.ds(pl.multiple_of(r * WIDE, WIDE), WIDE)
        ring[lax.rem(k, 2), band * WIDE : (band + 1) * WIDE, :] = jnp.dot(
            phi[at, :], cols_phi[lax.rem(j, 2)], preferred_element_type=jnp.float32
        )
        make(lax.rem(j + 1, wide), r)

    def emit(k):
        j, part = place(k)
        shift = start + j * WIDE - part * tall

        @pl.when((shift >= 0) & (shift < tall))
        def _():
            at = pl.ds(pl.multiple_of(shift, WIDE), WIDE)
            cols = pl.ds(pl.multiple_of(start + j * WIDE, WIDE), WIDE)
            slot = lax.rem(k, 2)
            ring[slot, at, :] = with_ridge(ring[slot, at, :], ridge[:, cols], 0, 0)

        ring_out(k).start()
        for blk in range(count):
            rows_out(blk, k).start()

    pair_steps(work, packed, panel, block_out, begin, beside, emit, size=size)
    tiles = size // TILE
    for k in range(tiles - 2, tiles):
        ring_out(k).wait()
    for blk in range(count):
        pltpu.make_async_copy(block_out.at[blk], out.at[blk], out_sem.at[blk]).wait()


def assemble(phi, sums, ridge, points, freqs, phases, size, scale):
    width, rows = phi.shape
    columns = freqs.shape[1]
    count = width // size
    outs = sums.shape[0]
    vmem = pl.BlockSpec(memory_space=pltpu.VMEM)
    hbm = pl.BlockSpec(memory_space=pltpu.HBM)
    return pl.pallas_call(
        functools.partial(assemble_body, count=count, size=size, scale=scale),
        out_shape=(
            jax.ShapeDtypeStruct((count, size, size), jnp.float32),
            jax.ShapeDtypeStruct((outs, width), jnp.float32),
            jax.ShapeDtypeStruct((width, columns), jnp.float32),
        ),
        in_specs=[vmem] * 6,
        out_specs=(hbm, vmem, hbm),
        scratch_shapes=[
            pltpu.VMEM((count, size, size), jnp.float32),
            pltpu.VMEM((count, size, size), jnp.float32),
            pltpu.VMEM((4, TILE, TILE), jnp.float32),
            pltpu.VMEM((count, TILE, TILE), jnp.float32),
            pltpu.VMEM((2, rows, WIDE), jnp.bfloat16),
            pltpu.VMEM((2, TILE // BAND * WIDE, WIDE), jnp.float32),
            pltpu.SemaphoreType.DMA((count,)),
            pltpu.SemaphoreType.DMA((2,)),
        ],
        compiler_params=pltpu.CompilerParams(vmem_limit_bytes=36 * MIB),
        cost_estimate=pl.CostEstimate(
            flops=30 * rows * width * size, bytes_accessed=8 * rows * width, transcendentals=0
        ),
        name="assemble",
    )(phi, sums, ridge, points, freqs, phases)


def near_shards(points, freqs, phase, ridge, targets):
    data_count, feat_count = lax.axis_size("dp"), lax.axis_size("feat")
    local_width = freqs.shape[1]
    tile_width = local_width * feat_count // data_count
    scale = math.sqrt(2.0 / (points.shape[0] * data_count))
    phi, points_all, col_freqs, turns, sums = spread(
        points, targets, phase, freqs, tile_width, scale
    )
    factors, projected, gram = assemble(
        phi, sums, ridge[None, :], points_all, col_freqs, turns, FB, scale
    )
    return gram, projected, factors.reshape(local_width, FB)


def lower_body(source, out, work, panel, sem, *, count, size):
    copy = pltpu.make_async_copy(source, work, sem)
    copy.start()
    copy.wait()
    factor_steps(work, panel, out, lambda k: None, count=count, size=size)


def lower_factors(blocks):
    count, size, _ = blocks.shape
    return pl.pallas_call(
        functools.partial(lower_body, count=count, size=size),
        out_shape=jax.ShapeDtypeStruct(blocks.shape, jnp.float32),
        in_specs=[pl.BlockSpec(memory_space=pl.ANY)],
        out_specs=pl.BlockSpec(memory_space=pltpu.VMEM),
        scratch_shapes=[
            pltpu.VMEM(blocks.shape, jnp.float32),
            pltpu.VMEM((count, TILE, 2 * TILE), jnp.float32),
            pltpu.SemaphoreType.DMA,
        ],
        compiler_params=pltpu.CompilerParams(vmem_limit_bytes=48 * MIB),
        name="lower_factors",
    )(blocks)


def wide_shards(points, freqs, phase, ridge, targets):
    data_count = lax.axis_size("dp")
    feat_count = lax.axis_size("feat")
    feat_index = lax.axis_index("feat")
    data_index = lax.axis_index("dp")
    local_width = freqs.shape[1]
    total_width = local_width * feat_count
    tile_width = total_width // data_count
    window = max(local_width, FB)
    window_start = feat_index * local_width // window * window
    row_start = feat_index * local_width
    col_start = data_index * tile_width
    scale = math.sqrt(2.0 / (points.shape[0] * data_count))
    points_all = lax.all_gather(points, "dp", axis=0, tiled=True)
    targets_all = lax.all_gather(targets, "dp", axis=1, tiled=True)
    freqs_all = lax.all_gather(freqs, "feat", axis=1, tiled=True)
    turns = phase * (0.5 / math.pi)
    turns_all, ridge_all = lax.all_gather(jnp.stack([turns, ridge]), "feat", axis=1, tiled=True)

    def features_at(start, width):
        return features(
            points_all,
            lax.dynamic_slice_in_dim(freqs_all, start, width, 1),
            lax.dynamic_slice_in_dim(turns_all, start, width, 0),
            scale,
        )

    window_phi = features_at(window_start, window)
    row_phi = lax.dynamic_slice_in_dim(window_phi, row_start - window_start, local_width, 1)
    window_ridge = lax.dynamic_slice_in_dim(ridge_all, window_start, window, 0)
    blocks = []
    for first in range(0, window, FB):
        part = window_phi[:, first : first + FB]
        block_ridge = window_ridge[first : first + FB, None]
        blocks.append(with_ridge(cross(part, part), block_ridge, 0, 0))
    factors_all = lower_factors(jnp.stack(blocks)).reshape(window, FB)
    factor_rows = lax.dynamic_slice_in_dim(factors_all, row_start - window_start, local_width, 0)
    col_phi = features_at(col_start, tile_width)
    gram_part = with_ridge(cross(row_phi, col_phi), ridge[:, None], row_start, col_start)
    projected = jnp.dot(targets_all, row_phi, preferred_element_type=jnp.float32)
    return gram_part, projected, factor_rows


def shards(points, freqs, phase, ridge, targets):
    local_width = freqs.shape[1]
    data_count, feat_count = lax.axis_size("dp"), lax.axis_size("feat")
    tile_width = local_width * feat_count // data_count
    near = (
        local_width == 2 * FB
        and local_width % tile_width == 0
        and tile_width % WIDE == 0
        and tile_width // WIDE * (local_width // WIDE) == FB // BAND
        and points.shape[0] * data_count % (local_width // WIDE) == 0
        and data_count % 2 == 0
        and feat_count == 4
    )
    return (near_shards if near else wide_shards)(points, freqs, phase, ridge, targets)


def solution(mesh):
    in_specs = (P("dp", None), P(None, "feat"), P("feat"), P("feat"), P(None, "dp"))
    out_specs = (P("feat", "dp"), P(None, "feat"), P("feat", None))
    return jax.shard_map(shards, mesh=mesh, in_specs=in_specs, out_specs=out_specs, check_vma=False)
```
